32 devices in a mesh: rows: 8 (over z, y), rep: 4 (over x, core).
Axes of the slice: x: 2, y: 2, z: 4, core: 2. Of those that a mesh axis runs over, the one named last changes fastest.
Arguments:
- tables: bfloat16 [16384, 128], P('rows'), may hold values from -0.5 to 0.5
- indices: int32 [512, 8, 8], P(('rows', 'rep')), may hold values from 0 to 2047
- bag_lengths: int32 [512, 8], P(('rows', 'rep')), may hold values from 1 to 8
- dense: bfloat16 [512, 13], P(('rows', 'rep')), may hold values from -6 to 6
- bottom_first: bfloat16 [13, 512], replicated, may hold values from -1.75 to 1.75
- bottom_second: bfloat16 [512, 256], replicated, may hold values from -0.375 to 0.375
- bottom_third: bfloat16 [256, 128], replicated, may hold values from -0.5 to 0.5
- top_first: bfloat16 [164, 1024], P(None, 'rep'), may hold values from -0.5 to 0.5
- top_second: bfloat16 [1024, 1024], P(None, 'rep'), may hold values from -0.25 to 0.25
- top_third: bfloat16 [1024, 512], P(None, 'rep'), may hold values from -0.25 to 0.25
- top_fourth: bfloat16 [512, 256], P(None, 'rep'), may hold values from -0.375 to 0.375
- top_last: bfloat16 [256], replicated, may hold values from -0.5 to 0.5
Outputs:
- logit: float32 [512], P(('rows', 'rep'))
The draws below stay inside these ranges and needn't reach their ends.
Inputs may be any that keep to these rules, and one draw needn't show every extreme that they name: `indices`: each entry is a row number within its own table; entries at positions of a bag at or past its length are ignored.
All inputs are finite; a program needn't handle non-finite values.
Results may differ from the reference program's by a relative error of at most 0.0076.
Values may be sent and summed in bfloat16 or wider, within the bound.
A program may use at most 64 MiB of HBM per device.

```python
import math
import jax
import jax.numpy as jnp
import numpy as np
from jax import lax

E = 128
DENSE = 13
H1 = 512
H2 = 256
T1 = 1024
T2 = 1024
T3 = 512
T4 = 256
TAB = 8
HOT = 8
TROWS = 2048
NPAIR = 36
BATCH = 512


def place_ends(values, own_key, least, largest):
    longest = values.shape.index(max(values.shape))
    spots = []
    for shift in (0, 1):
        where = [jax.random.randint(jax.random.fold_in(own_key, axis), (), 0, length) for axis, length in enumerate(values.shape)]
        where[longest] = (where[longest] + shift) % values.shape[longest]
        spots.append(tuple(where))
    return values.at[spots[0]].set(least).at[spots[1]].set(largest)


def levels(own_key, dims, split, smallest, top_value):
    def one(position, blocks):
        heights = jax.random.uniform(jax.random.fold_in(jax.random.fold_in(own_key, 6), position), (blocks,), jnp.float32, smallest / len(split), top_value / len(split))
        return jnp.repeat(jnp.exp(heights), dims[position] // blocks).reshape((-1,) + (1,) * (len(dims) - position - 1))

    level = one(*split[0])
    for cut in split[1:]:
        level = level * one(*cut)
    return level


def rank_table(amount, lean):
    weights = [(1 << 20) // math.isqrt(grade ** lean) + 1 for grade in range(1, amount + 1)]
    spread = 1 + sum(weights) // (1 << 30)
    return np.cumsum(np.array([max(1, weight // spread) for weight in weights]))


def skewed_ids(key, extent, number_of, lean):
    table = rank_table(number_of, lean)
    ticket = jax.random.randint(jax.random.fold_in(key, 1), extent, 0, int(table[number_of - 1]))
    grade = jnp.searchsorted(jnp.asarray(table, jnp.int32), ticket, side="right")
    return jax.random.permutation(jax.random.fold_in(key, 2), number_of)[grade].astype(jnp.int32)


def centred(key, dims, deviation, limit, cuts=(), kind=jnp.bfloat16):
    gain = levels(key, dims, cuts, -0.22, 0.18) if cuts else 1.0
    drawn = jax.random.normal(key, dims, jnp.float32) * deviation * gain
    return jnp.minimum(jnp.maximum(drawn, -limit), limit).astype(kind)


def setup_inputs(seed: int = 0) -> dict:
    keys = jax.random.split(jax.random.key(seed), 13)
    return {
        "tables": centred(keys[0], (TAB * TROWS, E), E ** -0.5, 0.5, ((0, 8),)),
        "indices": place_ends(skewed_ids(keys[1], (BATCH, TAB, HOT), TROWS, 2), jax.random.fold_in(keys[1], 3), 0, TROWS - 1).astype(jnp.int32),
        "bag_lengths": place_ends(jax.random.randint(keys[2], (BATCH, TAB), 1, HOT + 1), jax.random.fold_in(keys[2], 1), 1, HOT).astype(jnp.int32),
        "dense": centred(keys[3], (BATCH, DENSE), 1.0, 6.0, ((0, 32),)),
        "bottom_first": centred(keys[4], (DENSE, H1), DENSE ** -0.5, 1.75),
        "bottom_second": centred(keys[5], (H1, H2), (H1 // 2) ** -0.5, 0.375),
        "bottom_third": centred(keys[6], (H2, E), (H2 // 2) ** -0.5, 0.5),
        "top_first": centred(keys[7], (E + NPAIR, T1), (E + NPAIR) ** -0.5, 0.5, ((1, 4),)),
        "top_second": centred(keys[8], (T1, T2), (T1 // 2) ** -0.5, 0.25, ((1, 4),)),
        "top_third": centred(keys[9], (T2, T3), (T2 // 2) ** -0.5, 0.25, ((1, 4),)),
        "top_fourth": centred(keys[10], (T3, T4), (T3 // 2) ** -0.5, 0.375, ((1, 4),)),
        "top_last": centred(keys[11], (T4,), (T4 // 2) ** -0.5, 0.5),
    }


def interact(bottom_out, pooled):
    features = jnp.concatenate([bottom_out[None], pooled], axis=0)
    gram_matrix = jnp.einsum("ibe,jbe->bij", features, features, precision=lax.Precision.HIGHEST)
    left_ids, right_ids = np.triu_indices(TAB + 1, 1)
    pair_dots = gram_matrix[:, left_ids, right_ids]
    return jnp.concatenate([bottom_out, pair_dots], axis=1).astype(jnp.bfloat16)


def bottom_net(dense, bottom_first, bottom_second, bottom_third):
    lower_act = jax.nn.relu(jnp.dot(dense, bottom_first, preferred_element_type=jnp.float32)).astype(jnp.bfloat16)
    middle = jax.nn.relu(jnp.dot(lower_act, bottom_second, preferred_element_type=jnp.float32)).astype(jnp.bfloat16)
    return jax.nn.relu(jnp.dot(middle, bottom_third, preferred_element_type=jnp.float32))


def reference(tables, indices, bag_lengths, dense, bottom_first, bottom_second, bottom_third, top_first, top_second, top_third, top_fourth, top_last):
    def pool_one(carried):
        table_num, table_idx, table_len = carried
        row_ids = (table_num * TROWS + table_idx).astype(jnp.int32)
        live_mask = jnp.arange(HOT, dtype=jnp.int32)[None, :] < table_len[:, None]
        picked = jnp.take(tables, row_ids, axis=0).astype(jnp.float32)
        return jnp.sum(jnp.where(live_mask[:, :, None], picked, jnp.zeros_like(picked)), axis=1)

    pooled = lax.map(pool_one, (jnp.arange(TAB, dtype=jnp.int32), jnp.transpose(indices, (1, 0, 2)), jnp.transpose(bag_lengths)))
    bottom_out = bottom_net(dense, bottom_first, bottom_second, bottom_third)
    activation = interact(bottom_out, pooled)
    for weight_mat in (top_first, top_second, top_third, top_fourth):
        activation = jax.nn.relu(jnp.dot(activation, weight_mat, preferred_element_type=jnp.float32)).astype(jnp.bfloat16)
    return jnp.dot(activation, top_last, preferred_element_type=jnp.float32)
```

```python
import functools

import jax
import jax.numpy as jnp
from jax import lax
from jax.experimental import pallas as pl
from jax.experimental.pallas import tpu as pltpu
from jax.sharding import PartitionSpec as P

TAB = 8
HOT = 8
LANES = 128
MESH = pl.DeviceIdType.MESH
BF16 = jnp.bfloat16
F32 = jnp.float32


def flip(k, offset):
    bit = 1
    while bit <= offset:
        if offset & bit:
            k = k + bit - 2 * bit * ((k // bit) % 2)
        bit *= 2
    return k


def dot(a, b):
    return jnp.dot(a, b, preferred_element_type=F32)


def dot_t(a, b):
    return lax.dot_general(a, b, (((1,), (1,)), ((), ())), preferred_element_type=F32)


def run_half(lookup, base, count):
    if count == 4:
        lookup(base)
    else:
        pl.loop(0, count // 4)(lambda g: lookup(base + 4 * g))


def relu_round(x):
    return jnp.maximum(x, 0.0).astype(BF16)


def kernel(
    D,
    R,
    tables,
    indices_h,
    lengths_h,
    dense_h,
    bottom_first_h,
    bottom_second_h,
    bottom_third_h,
    top_first,
    top_second,
    top_third,
    top_fourth,
    top_last_h,
    out,
    indices,
    bag_lengths,
    dense,
    bottom_first,
    bottom_second,
    bottom_third,
    top_last,
    table_v,
    w1,
    w2,
    w3,
    w4,
    out_idx,
    recv_idx,
    counts,
    part,
    recv_pool,
    recv_top,
    act1,
    act2,
    recv_act2,
    local_sem,
    e1_send,
    e1_recv,
    e2_send,
    e2_recv,
    e3_send,
    e3_recv,
    e4_send,
    e4_recv,
    w_send,
    w_recv,
):
    B = indices.shape[2]
    rows = tables.shape[0]
    per_table = D // TAB
    me = lax.axis_index("rows")
    k = lax.axis_index("rep")

    barrier = pltpu.get_barrier_semaphore()
    for d in range(1, D):
        pl.semaphore_signal(
            barrier, inc=1, device_id=(lax.rem(me + d, D), k), device_id_type=MESH
        )
    for o in range(1, R):
        pl.semaphore_signal(barrier, inc=1, device_id=(me, flip(k, o)), device_id_type=MESH)

    small = [
        pltpu.make_async_copy(indices_h, indices, local_sem.at[5]),
        pltpu.make_async_copy(lengths_h, bag_lengths, local_sem.at[6]),
        pltpu.make_async_copy(dense_h, dense, local_sem.at[7]),
        pltpu.make_async_copy(bottom_first_h, bottom_first, local_sem.at[8]),
        pltpu.make_async_copy(bottom_second_h, bottom_second, local_sem.at[9]),
        pltpu.make_async_copy(bottom_third_h, bottom_third, local_sem.at[10]),
        pltpu.make_async_copy(top_last_h, top_last, local_sem.at[11]),
    ]
    local = [
        pltpu.make_async_copy(tables, table_v, local_sem.at[0]),
        pltpu.make_async_copy(top_first, w1.at[k], local_sem.at[1]),
        pltpu.make_async_copy(top_second, w2, local_sem.at[2]),
        pltpu.make_async_copy(top_third, w3.at[k], local_sem.at[3]),
        pltpu.make_async_copy(top_fourth, w4.at[k], local_sem.at[4]),
    ]
    for copy in small + local:
        copy.start()

    small[0].wait()
    small[1].wait()
    lens = bag_lengths[...]
    out_idx[...] = jnp.concatenate(
        [jnp.where(lens > s, indices[:, s, :], -1) for s in range(HOT)], axis=1
    ).reshape(TAB, 1, B * HOT)

    pl.semaphore_wait(barrier, D - 1 + R - 1)

    sends = []

    def send(src, dst, ssem, rsem, device):
        copy = pltpu.make_async_remote_copy(
            src_ref=src,
            dst_ref=dst,
            send_sem=ssem,
            recv_sem=rsem,
            device_id=device,
            device_id_type=MESH,
        )
        copy.start()
        sends.append(copy)
        return copy

    first = {}
    for d in reversed(range(1, D)):
        peer = flip(me, d)
        first[d] = send(
            out_idx.at[peer // per_table], recv_idx.at[me], e1_send.at[d], e1_recv.at[d], (peer, k)
        )
    recv_idx[me] = out_idx[me // per_table]

    mine = (top_first, top_third, top_fourth)
    whole = (w1, w3, w4)
    arriving = {}
    stages = []
    held = [0]
    bit = R // 2
    while bit:
        stages.append([(bit, h) for h in held])
        held = held + [h ^ bit for h in held]
        bit //= 2

    def weight_send(array, bit, h):
        block = flip(k, h)
        src = mine[array] if h == 0 else whole[array].at[block]
        arriving[array, h ^ bit] = send(
            src,
            whole[array].at[block],
            w_send.at[array * R + (h ^ bit)],
            w_recv.at[array * R + (h ^ bit)],
            (me, flip(k, bit)),
        )

    for array in range(3):
        for stage in stages:
            for bit, h in stage:
                if h == 0:
                    weight_send(array, bit, h)

    got = set()

    def weight_forward(array):
        for stage in stages:
            for bit, h in stage:
                if h != 0:
                    if (array, h) not in got:
                        arriving[array, h].wait_recv()
                        got.add((array, h))
                    weight_send(array, bit, h)

    def weight_finish(array):
        for o in range(1, R):
            if (array, o) not in got:
                arriving[array, o].wait_recv()
                got.add((array, o))

    for copy in small[2:]:
        copy.wait()
    lower = relu_round(dot(dense[...], bottom_first[...]))
    middle = relu_round(dot(lower, bottom_second[...]))
    bottom_out = jnp.maximum(dot(middle, bottom_third[...]), 0.0)

    local[0].wait()

    offset = (me % per_table) * rows
    lanes = lax.broadcasted_iota(jnp.int32, (16, LANES), 1).astype(F32).astype(BF16)
    one, zero = jnp.ones((16, LANES), BF16), jnp.zeros((16, LANES), BF16)
    half = B // 2

    def lookup(base):
        rows4 = recv_idx[pl.ds(base, 4)].reshape(4, B * HOT) - offset
        wanted = jnp.concatenate([rows4, pltpu.roll(rows4, B * HOT - half, 1)], axis=0)
        blocks = rows // LANES
        for pair in range(half // 2):
            totals = [jnp.zeros((16, LANES), BF16)] * blocks
            for s in range(HOT):
                j = B * s + 2 * pair
                entry = jnp.concatenate([wanted[:, j : j + 1], wanted[:, j + 1 : j + 2]], axis=0)
                entry = jnp.broadcast_to(entry, (16, LANES))
                high_part = (entry >> 7).astype(F32).astype(BF16)
                low_part = (entry & (LANES - 1)).astype(F32).astype(BF16)
                hit = jnp.where(low_part == lanes, one, zero)
                for n in range(blocks):
                    here = jnp.where(high_part == jnp.asarray(n, BF16), hit, zero)
                    totals[n] = totals[n] + here
            for n in range(blocks):
                counts[16 * pair : 16 * pair + 16, n * LANES : (n + 1) * LANES] = totals[n]
        partial = dot(counts[...], table_v[...])
        for b in range(half):
            part[pl.ds(base, 4), b, :] = partial[8 * b : 8 * b + 4, :]
            part[pl.ds(base, 4), b + half, :] = partial[8 * b + 4 : 8 * b + 8, :]

    second = []

    def second_send(d):
        peer = flip(me, d)
        second.append(
            send(part.at[peer], recv_pool.at[me], e2_send.at[d], e2_recv.at[d], (peer, k))
        )

    low, high = D // 2, D
    for d in range(1, low):
        first[d].wait_recv()
    run_half(lookup, me // low * low, low)
    for d in range(1, low):
        second_send(d)
    for d in range(low, high):
        first[d].wait_recv()
    run_half(lookup, (1 - me // low) * low, low)
    for d in range(low, high):
        second_send(d)
    recv_pool[me] = part[me]
    weight_forward(0)
    for copy in second:
        copy.wait_recv()

    features = [bottom_out]
    for t in range(TAB):
        pooled = recv_pool[t * per_table]
        for i in range(1, per_table):
            pooled = pooled + recv_pool[t * per_table + i]
        features.append(pooled)
    E = bottom_out.shape[1]
    lane = lax.broadcasted_iota(jnp.int32, (B, E), 1)
    dots = jnp.zeros((B, E), F32)
    p = 0
    for i in range(TAB + 1):
        for j in range(i + 1, TAB + 1):
            value = jnp.sum(features[i] * features[j], axis=1, keepdims=True)
            dots = jnp.where(lane == p, value, dots)
            p += 1
    recv_top[k] = jnp.concatenate([bottom_out, dots], axis=1).astype(BF16)

    third = [
        send(recv_top.at[k], recv_top.at[k], e3_send.at[o], e3_recv.at[o], (me, flip(k, o)))
        for o in range(1, R)
    ]
    weight_finish(0)
    weight_forward(1)
    weight_forward(2)
    for copy in local[1:]:
        copy.wait()
    for copy in third:
        copy.wait_recv()

    top_in = recv_top[...].reshape(R * B, 2 * E)
    n1 = w1.shape[2]
    for n in range(R):
        act1[:, n * n1 : (n + 1) * n1] = relu_round(
            dot(top_in[:, :E], w1[n, :E, :]) + dot(top_in[:, E : E + p], w1[n, E:, :])
        )
    act2[...] = relu_round(dot(act1[...], w2[...])).reshape(act2.shape)

    fourth = [
        send(
            act2.at[flip(k, o)], recv_act2.at[k], e4_send.at[o], e4_recv.at[o], (me, flip(k, o))
        )
        for o in range(1, R)
    ]
    recv_act2[k] = act2[k]
    weight_finish(1)
    weight_finish(2)
    for copy in fourth:
        copy.wait_recv()

    third_in = jnp.concatenate([recv_act2[n] for n in range(R)], axis=1)
    fourth_in = jnp.concatenate([relu_round(dot(third_in, w3[n])) for n in range(R)], axis=1)
    last_in = jnp.concatenate([relu_round(dot_t(fourth_in, w4[n])) for n in range(R)], axis=1)
    out[...] = dot_t(top_last[...].reshape(1, -1), last_in).reshape(B)
    for copy in sends:
        copy.wait_send()


def body(*args):
    (tables, indices, bag_lengths, dense, b1, b2, b3, t1, t2, t3, t4, last) = args
    D = lax.axis_size("rows")
    R = lax.axis_size("rep")
    B = indices.shape[0]
    indices = jnp.transpose(indices, (1, 2, 0))
    bag_lengths = jnp.transpose(bag_lengths)
    t4 = jnp.transpose(t4)
    E = tables.shape[1]
    vmem = pl.BlockSpec(memory_space=pltpu.VMEM)
    hbm = pl.BlockSpec(memory_space=pl.ANY)
    dma = pltpu.SemaphoreType.DMA
    result = pl.pallas_call(
        functools.partial(kernel, D, R),
        out_shape=pltpu.VMEM((B,), F32),
        in_specs=[hbm] * 12,
        out_specs=vmem,
        scratch_shapes=[
            pltpu.VMEM(indices.shape, jnp.int32),
            pltpu.VMEM(bag_lengths.shape, jnp.int32),
            pltpu.VMEM(dense.shape, BF16),
            pltpu.VMEM(b1.shape, BF16),
            pltpu.VMEM(b2.shape, BF16),
            pltpu.VMEM(b3.shape, BF16),
            pltpu.VMEM(last.shape, BF16),
            pltpu.VMEM(tables.shape, BF16),
            pltpu.VMEM((R,) + t1.shape, BF16),
            pltpu.VMEM(t2.shape, BF16),
            pltpu.VMEM((R,) + t3.shape, BF16),
            pltpu.VMEM((R,) + t4.shape, BF16),
            pltpu.VMEM((TAB, 1, B * HOT), jnp.int32),
            pltpu.VMEM((D, 1, B * HOT), jnp.int32),
            pltpu.VMEM((4 * B, tables.shape[0]), BF16),
            pltpu.VMEM((D, B, E), F32),
            pltpu.VMEM((D, B, E), F32),
            pltpu.VMEM((R, B, 2 * E), BF16),
            pltpu.VMEM((R * B, R * t1.shape[1]), BF16),
            pltpu.VMEM((R, B, t2.shape[1]), BF16),
            pltpu.VMEM((R, B, t2.shape[1]), BF16),
            dma((12,)),
            dma((D,)),
            dma((D,)),
            dma((D,)),
            dma((D,)),
            dma((R,)),
            dma((R,)),
            dma((R,)),
            dma((R,)),
            dma((3 * R,)),
            dma((3 * R,)),
        ],
        compiler_params=pltpu.CompilerParams(collective_id=0, has_side_effects=True),
    )(tables, indices, bag_lengths, dense, b1, b2, b3, t1, t2, t3, t4, last)
    return result


def solution(mesh):
    placed = (
        P("rows", None),
        P(("rows", "rep"), None, None),
        P(("rows", "rep"), None),
        P(("rows", "rep"), None),
        P(),
        P(),
        P(),
        P(None, "rep"),
        P(None, "rep"),
        P(None, "rep"),
        P(None, "rep"),
        P(),
    )
    return jax.shard_map(
        body, mesh=mesh, in_specs=placed, out_specs=P(("rows", "rep")), check_vma=False
    )
```

```python
import functools

import jax
import jax.numpy as jnp
from jax import lax
from jax.experimental import pallas as pl
from jax.experimental.pallas import tpu as pltpu
from jax.sharding import PartitionSpec as P

TAB = 8
HOT = 8
LANES = 128
PACK = 16
SHIFT = 4
CHUNK = 256
SPAN = 65536
(S_IDX, R_IDX, S_DENSE, R_DENSE, S_W1, R_W1, S_W2, R_W2) = range(7, 15)
(S_E1, R_E1A, R_E1B, S_E2, R_E2, S_E3, R_E3, S_E4, R_E4) = range(15, 24)
S_OWN, S_FORWARD, R_DOWN, R_ACROSS = 24, 26, 28, 30
MESH = pl.DeviceIdType.MESH
BF16 = jnp.bfloat16
F32 = jnp.float32


def flip(k, offset):
    bit = 1
    while bit <= offset:
        if offset & bit:
            k = k + bit - 2 * bit * ((k // bit) % 2)
        bit *= 2
    return k


def dot(a, b):
    return jnp.dot(a, b, preferred_element_type=F32)


def dot_t(a, b):
    return lax.dot_general(a, b, (((1,), (1,)), ((), ())), preferred_element_type=F32)


def relu_round(x):
    return jnp.maximum(x, 0.0).astype(BF16)


def kernel(
    D,
    R,
    tables,
    indices_h,
    lengths_h,
    dense_h,
    bottom_first_h,
    bottom_second_h,
    bottom_third_h,
    top_first,
    top_second,
    top_third,
    top_fourth,
    top_last_h,
    out,
    indices,
    bag_lengths,
    dense,
    bottom_first,
    bottom_second,
    bottom_third,
    top_last,
    table_v,
    table_t,
    w1,
    w2,
    w3,
    w4,
    own_idx,
    pair_idx,
    out_idx,
    recv_idx,
    part,
    recv_pool,
    recv_top,
    act1,
    act2,
    recv_act2,
    go,
    sem,
):
    B = indices.shape[2]
    rows, E = tables.shape
    X = R // 2
    group = LANES // (2 * B)
    per_table = D // TAB
    me = lax.axis_index("rows")
    k = lax.axis_index("rep")
    core = k % 2
    x = k // 2
    mate = flip(k, 1)
    low, high = D // 2, D

    barrier = pltpu.get_barrier_semaphore()

    def greet(device):
        pl.semaphore_signal(barrier, inc=1, device_id=device, device_id_type=MESH)

    def local(src, dst, i):
        copy = pltpu.make_async_copy(src, dst, sem.at[i])
        copy.start()
        return copy

    def remote(src, dst, ssem, rsem, device):
        return pltpu.make_async_remote_copy(
            src_ref=src,
            dst_ref=dst,
            send_sem=sem.at[ssem],
            recv_sem=sem.at[rsem],
            device_id=device,
            device_id_type=MESH,
        )

    def send(src, dst, ssem, rsem, device):
        remote(src, dst, ssem, rsem, device).start()

    def arrive(dst, rsem):
        remote(dst, dst, rsem, rsem, (me, mate)).wait_recv()

    def sent(src, ssem):
        remote(src, src, ssem, ssem, (me, mate)).wait_send()

    def sent_blocks(stack, count, ssem):
        while count:
            now = min(count, stack.shape[0])
            sent(stack.at[pl.ds(0, now)], ssem)
            count -= now

    def own_tile():
        lens = bag_lengths[...].reshape(TAB, 1, B)
        slot = lax.broadcasted_iota(jnp.int32, (TAB, HOT, B), 1)
        own_idx[...] = jnp.full(own_idx.shape, -1, jnp.int32)
        own_idx[:, :, :B] = jnp.where(slot < lens, indices[...], -1)
        place = B * (2 * (me % group) + core)
        slot = lax.broadcasted_iota(jnp.int32, (HOT, LANES), 0)
        tiles = []
        for t in range(TAB):
            entry = own_idx[t]
            many = jnp.ones(entry.shape, jnp.int32)
            again = entry < 0
            for r in range(1, HOT):
                other = pltpu.roll(entry, r, 0)
                same = entry == other
                many = many + jnp.where(same, 1, 0)
                again = jnp.logical_or(again, jnp.logical_and(same, slot >= r))
            entry = jnp.where(again, -1, entry + many * SPAN)
            tiles.append(pltpu.roll(entry, place, 1))
        return jnp.stack(tiles)

    halves = (top_third, top_fourth)
    whole = (w3, w4)

    def finish():
        third_in = jnp.concatenate([recv_act2[n] for n in range(X)], axis=1)
        fourth_in = jnp.concatenate([relu_round(dot(third_in, w3[n])) for n in range(R)], axis=1)
        last_in = jnp.concatenate([relu_round(dot_t(fourth_in, w4[n])) for n in range(R)], axis=1)
        out[...] = dot_t(top_last[...].reshape(1, -1), last_in).reshape(B)

    greet((me, mate))
    for o in range(1, X):
        greet((me, 2 * flip(x, o) + 1))
    get_idx = local(indices_h, indices, 0)
    get_len = local(lengths_h, bag_lengths, 1)

    @pl.when(core == 0)
    def follower():
        later = [
            local(top_third, w3.at[k], 2),
            local(top_fourth, w4.at[k], 3),
            local(top_last_h, top_last, 4),
        ]
        get_idx.wait()
        get_len.wait()
        pair_idx[...] = own_tile()
        pl.semaphore_wait(barrier, 1)
        up = (me, mate)
        send(pair_idx, pair_idx, S_IDX, R_IDX, up)
        send(dense_h, dense.at[0], S_DENSE, R_DENSE, up)
        send(top_first, w1.at[k], S_W1, R_W1, up)
        send(top_second, w2.at[0], S_W2, R_W2, up)
        for a in range(2):
            send(halves[a], whole[a].at[k], S_OWN + a, R_DOWN + a, up)
        pl.semaphore_wait(go, 1)

        def over(a, src, block, ssem, h):
            for o in range(1, X):
                send(
                    src,
                    whole[a].at[block],
                    ssem,
                    R_ACROSS + a * R + 2 * o + h,
                    (me, flip(k, 2 * o)),
                )

        for o in range(1, X):
            send(top_first, w1.at[k], S_W1, R_W1, (me, flip(k, 2 * o + 1)))
        for a in range(2):
            over(a, halves[a], k, S_OWN + a, 0)
        for a in range(2):
            arrive(whole[a].at[mate], R_ACROSS + a * R)
            over(a, whole[a].at[mate], mate, S_FORWARD + a, 1)
        for h in range(2):
            for a in range(2):
                for o in range(1, X):
                    block = whole[a].at[flip(k, 2 * o + h)]
                    arrive(block, R_ACROSS + a * R + 2 * o + h)
                    send(block, block, S_FORWARD + a, R_DOWN + a, up)
        for copy in later:
            copy.wait()
        arrive(recv_act2, R_E4)
        finish()
        sent(pair_idx, S_IDX)
        sent(dense.at[0], S_DENSE)
        sent(w2.at[0], S_W2)
        sent_blocks(w1, X, S_W1)
        for a in range(2):
            sent_blocks(whole[a], X, S_OWN + a)
            sent_blocks(whole[a], 3 * (X - 1), S_FORWARD + a)

    @pl.when(core == 1)
    def leader():
        for d in range(1, D):
            greet((flip(me, d), k))
        get_dense = local(dense_h, dense.at[1], 2)
        get_bottom = [
            local(bottom_first_h, bottom_first, 3),
            local(bottom_second_h, bottom_second, 4),
            local(bottom_third_h, bottom_third, 5),
        ]
        get_table = local(tables, table_v, 6)
        get_idx.wait()
        get_len.wait()
        later = [local(top_second, w2.at[1], 0), local(top_first, w1.at[k], 1)]
        mine = own_tile()
        pl.semaphore_wait(barrier, D - 1 + 1 + 2 * (X - 1))
        arrive(pair_idx, R_IDX)
        out_idx[...] = jnp.maximum(mine, pair_idx[...])

        for d in reversed(range(1, D)):
            peer = flip(me, d)
            send(
                out_idx.at[peer // per_table],
                recv_idx.at[me],
                S_E1,
                R_E1A if d < low else R_E1B,
                (peer, k),
            )
        pl.semaphore_signal(go, inc=1, device_id=(me, mate), device_id_type=MESH)
        recv_idx[me] = out_idx[me // per_table]
        for o in range(1, X):
            send(top_first, w1.at[k], S_W1, R_W1, (me, flip(k, 2 * o)))
        for a in range(2):
            send(halves[a], whole[a].at[k], S_OWN + a, R_ACROSS + a * R, (me, mate))

        get_table.wait()
        table_t[...] = table_v[...].T

        get_dense.wait()
        for copy in get_bottom:
            copy.wait()
        later += [
            local(top_third, w3.at[k], 2),
            local(top_fourth, w4.at[k], 3),
            local(top_last_h, top_last, 4),
        ]
        arrive(dense.at[0], R_DENSE)
        lower = relu_round(dot(dense[...].reshape(2 * B, -1), bottom_first[...]))
        middle = relu_round(dot(lower, bottom_second[...]))
        bottom_out = jnp.maximum(dot(middle, bottom_third[...]), 0.0)

        offset = (me % per_table) * rows
        sub = lax.broadcasted_iota(jnp.int32, (PACK, LANES), 0)
        zero = jnp.zeros((PACK, LANES), BF16)

        def lookup(g):
            base = group * g
            entry = recv_idx[base]
            for i in range(1, group):
                entry = jnp.maximum(entry, recv_idx[base + i])
            codes, counts = [], []
            for s in range(HOT):
                row = jnp.broadcast_to(entry[s : s + 1, :], (PACK, LANES))
                spot = (row & (SPAN - 1)) - offset
                hit = jnp.logical_and((spot & (PACK - 1)) == sub, row >= 0)
                codes.append(jnp.where(hit, spot >> SHIFT, -1).astype(F32).astype(BF16))
                counts.append((row // SPAN).astype(F32).astype(BF16))
            partial = jnp.zeros((E, LANES), F32)
            for c in range(rows // CHUNK):
                chunk = []
                for n in range(c * CHUNK // PACK, (c + 1) * CHUNK // PACK):
                    total = zero
                    for code, count in zip(codes, counts):
                        total = jnp.where(code == jnp.asarray(n, BF16), count, total)
                    chunk.append(total)
                partial = partial + dot(
                    table_t[:, c * CHUNK : (c + 1) * CHUNK], jnp.concatenate(chunk, axis=0)
                )
            part[pl.ds(base, group)] = partial.T.reshape(group, 2 * B, E)

        def run(base, count):
            if count == group:
                lookup(base // group)
            else:
                pl.loop(0, count // group)(lambda g: lookup(base // group + g))

        def second_send(d):
            peer = flip(me, d)
            send(part.at[peer], recv_pool.at[me], S_E2, R_E2, (peer, k))

        arrive(recv_idx.at[pl.ds(0, low - 1)], R_E1A)
        run(me // low * low, low)
        for d in range(1, low):
            second_send(d)
        arrive(recv_idx.at[pl.ds(0, low)], R_E1B)
        run((1 - me // low) * low, low)
        for d in range(low, high):
            second_send(d)
        recv_pool[me] = part[me]
        arrive(recv_pool.at[pl.ds(0, D - 1)], R_E2)

        features = [bottom_out]
        for t in range(TAB):
            pooled = recv_pool[t * per_table]
            for i in range(1, per_table):
                pooled = pooled + recv_pool[t * per_table + i]
            features.append(pooled)
        lane = lax.broadcasted_iota(jnp.int32, (2 * B, E), 1)
        dots = jnp.zeros((2 * B, E), F32)
        p = 0
        for i in range(TAB + 1):
            for j in range(i + 1, TAB + 1):
                value = jnp.sum(features[i] * features[j], axis=1, keepdims=True)
                dots = jnp.where(lane == p, value, dots)
                p += 1
        recv_top[x] = jnp.concatenate([bottom_out, dots], axis=1).astype(BF16)

        for o in range(1, X):
            send(recv_top.at[x], recv_top.at[x], S_E3, R_E3, (me, flip(k, 2 * o)))
        for copy in later:
            copy.wait()
        arrive(w1.at[pl.ds(0, R - 1)], R_W1)
        arrive(w2.at[0], R_W2)
        if X > 1:
            arrive(recv_top.at[pl.ds(0, X - 1)], R_E3)

        top_in = recv_top[...].reshape(R * B, 2 * E)
        n1, n2 = w1.shape[2], w2.shape[2]
        for n in range(R):
            act1[:, n * n1 : (n + 1) * n1] = relu_round(
                dot(top_in[:, :E], w1[n, :E, :]) + dot(top_in[:, E : E + p], w1[n, E:, :])
            )
        for j in range(2):
            act2[:, :, j * n2 : (j + 1) * n2] = relu_round(dot(act1[...], w2[j])).reshape(
                R, B, n2
            )
        for o in range(1, X):
            for h in range(2):
                to = flip(k, 2 * o + h)
                send(act2.at[to], recv_act2.at[x], S_E4, R_E4, (me, to))
        send(act2.at[mate], recv_act2.at[x], S_E4, R_E4, (me, mate))
        recv_act2[x] = act2[k]
        for a in range(2):
            arrive(whole[a].at[pl.ds(0, R - 1)], R_DOWN + a)
        if X > 1:
            arrive(recv_act2.at[pl.ds(0, X - 1)], R_E4)
        finish()
        sent(recv_idx.at[pl.ds(0, D - 1)], S_E1)
        sent(part.at[pl.ds(0, D - 1)], S_E2)
        for a in range(2):
            sent(whole[a].at[k], S_OWN + a)
        sent(act2.at[pl.ds(0, R - 1)], S_E4)
        if X > 1:
            sent_blocks(w1, X - 1, S_W1)
            sent(recv_top.at[pl.ds(0, X - 1)], S_E3)


def body(*args):
    (tables, indices, bag_lengths, dense, b1, b2, b3, t1, t2, t3, t4, last) = args
    D = lax.axis_size("rows")
    R = lax.axis_size("rep")
    B = indices.shape[0]
    indices = jnp.transpose(indices, (1, 2, 0))
    bag_lengths = jnp.transpose(bag_lengths)
    t4 = jnp.transpose(t4)
    rows, E = tables.shape
    X = R // 2
    hbm = pl.BlockSpec(memory_space=pl.ANY)
    tile = pltpu.VMEM((TAB, HOT, LANES), jnp.int32)
    result = pl.pallas_call(
        functools.partial(kernel, D, R),
        out_shape=pltpu.VMEM((B,), F32),
        in_specs=[hbm] * 12,
        out_specs=pl.BlockSpec(memory_space=pltpu.VMEM),
        scratch_shapes=[
            pltpu.VMEM(indices.shape, jnp.int32),
            pltpu.VMEM(bag_lengths.shape, jnp.int32),
            pltpu.VMEM((2,) + dense.shape, BF16),
            pltpu.VMEM(b1.shape, BF16),
            pltpu.VMEM(b2.shape, BF16),
            pltpu.VMEM(b3.shape, BF16),
            pltpu.VMEM(last.shape, BF16),
            pltpu.VMEM((rows, E), BF16),
            pltpu.VMEM((E, rows), BF16),
            pltpu.VMEM((R,) + t1.shape, BF16),
            pltpu.VMEM((2,) + t2.shape, BF16),
            pltpu.VMEM((R,) + t3.shape, BF16),
            pltpu.VMEM((R,) + t4.shape, BF16),
            tile,
            tile,
            tile,
            pltpu.VMEM((D, HOT, LANES), jnp.int32),
            pltpu.VMEM((D, 2 * B, E), F32),
            pltpu.VMEM((D, 2 * B, E), F32),
            pltpu.VMEM((X, 2 * B, 2 * E), BF16),
            pltpu.VMEM((R * B, R * t1.shape[1]), BF16),
            pltpu.VMEM((R, B, 2 * t2.shape[1]), BF16),
            pltpu.VMEM((X, B, 2 * t2.shape[1]), BF16),
            pltpu.SemaphoreType.REGULAR,
            pltpu.SemaphoreType.DMA((R_ACROSS + 2 * R,)),
        ],
        compiler_params=pltpu.CompilerParams(collective_id=0, has_side_effects=True),
    )(tables, indices, bag_lengths, dense, b1, b2, b3, t1, t2, t3, t4, last)
    return result


def solution(mesh):
    placed = (
        P("rows", None),
        P(("rows", "rep"), None, None),
        P(("rows", "rep"), None),
        P(("rows", "rep"), None),
        P(),
        P(),
        P(),
        P(None, "rep"),
        P(None, "rep"),
        P(None, "rep"),
        P(None, "rep"),
        P(),
    )
    return jax.shard_map(
        body, mesh=mesh, in_specs=placed, out_specs=P(("rows", "rep")), check_vma=False
    )
```

```python
import functools

import jax
import jax.numpy as jnp
from jax import lax
from jax.experimental import pallas as pl
from jax.experimental.pallas import tpu as pltpu
from jax.sharding import PartitionSpec as P

TAB = 8
HOT = 8
LANES = 128
PACK = 16
SHIFT = 4
CHUNK = 256
EARLY = 4
SPAN = 65536
S_DENSE, S_W1, S_W3, S_OWN, S_E4, R_IDX, R_DENSE, R_W1, R_W2, R_W3, R_E4, R_DOWN = range(7, 19)
S_E1, S_E2, S_E3, R_E1A, R_E1B, R_E2, R_E2X, R_E3 = range(19, 27)
S_IDX, S_W2, S_FORWARD, R_ACROSS = range(19, 23)
MESH = pl.DeviceIdType.MESH
BF16 = jnp.bfloat16
F32 = jnp.float32


def flip(k, offset):
    bit = 1
    while bit <= offset:
        if offset & bit:
            k = k + bit - 2 * bit * ((k // bit) % 2)
        bit *= 2
    return k


def dot(a, b):
    return jnp.dot(a, b, preferred_element_type=F32)


def dot_t(a, b):
    return lax.dot_general(a, b, (((1,), (1,)), ((), ())), preferred_element_type=F32)


def relu_round(x):
    return jnp.maximum(x, 0.0).astype(BF16)


def kernel(
    D,
    R,
    tables,
    indices_h,
    lengths_h,
    dense_h,
    bottom_first_h,
    bottom_second_h,
    bottom_third_h,
    top_first,
    top_second,
    top_third,
    top_fourth,
    top_last_h,
    out,
    indices,
    bag_lengths,
    dense,
    bottom_first,
    bottom_second,
    bottom_third,
    top_last,
    last,
    table_v,
    table_t,
    w1,
    w2,
    w3,
    w4,
    own_idx,
    pair_idx,
    out_idx,
    recv_idx,
    part,
    recv_pool,
    recv_dots,
    bottom,
    first,
    act1,
    third,
    recv_third,
    sem,
):
    B = indices.shape[2]
    rows, E = tables.shape
    X = R // 2
    group = LANES // (2 * B)
    per_table = D // TAB
    me = lax.axis_index("rows")
    k = lax.axis_index("rep")
    core = k % 2
    x = k // 2
    mate = flip(k, 1)
    low, high = D // 2, D
    early = max(D // EARLY, 1)

    barrier = pltpu.get_barrier_semaphore()

    def greet(device):
        pl.semaphore_signal(barrier, inc=1, device_id=device, device_id_type=MESH)

    def local(src, dst, i):
        copy = pltpu.make_async_copy(src, dst, sem.at[i])
        copy.start()
        return copy

    def remote(src, dst, ssem, rsem, device):
        return pltpu.make_async_remote_copy(
            src_ref=src,
            dst_ref=dst,
            send_sem=sem.at[ssem],
            recv_sem=sem.at[rsem],
            device_id=device,
            device_id_type=MESH,
        )

    def send(src, dst, ssem, rsem, device):
        remote(src, dst, ssem, rsem, device).start()

    def arrive(dst, rsem):
        remote(dst, dst, rsem, rsem, (me, mate)).wait_recv()

    def sent(src, ssem):
        remote(src, src, ssem, ssem, (me, mate)).wait_send()

    def sent_blocks(stack, count, ssem):
        while count:
            now = min(count, stack.shape[0])
            sent(stack.at[pl.ds(0, now)], ssem)
            count -= now

    def own_tile():
        lens = bag_lengths[...].reshape(TAB, 1, B)
        slot = lax.broadcasted_iota(jnp.int32, (TAB, HOT, B), 1)
        own_idx[...] = jnp.full(own_idx.shape, -1, jnp.int32)
        own_idx[:, :, :B] = jnp.where(slot < lens, indices[...], -1)
        place = B * (2 * (me % group) + core)
        slot = lax.broadcasted_iota(jnp.int32, (HOT, LANES), 0)
        tiles = []
        for t in range(TAB):
            entry = own_idx[t]
            many = jnp.ones(entry.shape, jnp.int32)
            again = entry < 0
            for r in range(1, HOT):
                other = pltpu.roll(entry, r, 0)
                same = entry == other
                many = many + jnp.where(same, 1, 0)
                again = jnp.logical_or(again, jnp.logical_and(same, slot >= r))
            entry = jnp.where(again, -1, entry + many * SPAN)
            tiles.append(pltpu.roll(entry, place, 1))
        return jnp.stack(tiles)

    deep = w3.shape[1]

    def strip(o):
        return top_third.at[pl.ds(pl.multiple_of(flip(x, o) * deep, deep), deep)]

    def finish():
        total = recv_third[0]
        for n in range(1, X):
            total = total + recv_third[n]
        fourth_in = relu_round(total)
        last_in = relu_round(dot_t(w4[...].reshape(last.shape[0], -1), fourth_in))
        out[...] = jnp.sum(last_in.astype(F32) * last[...], axis=0)

    def last_column():
        row = top_last[...].reshape(1, -1).astype(F32)
        last[...] = jnp.broadcast_to(row, (B, row.shape[1])).T

    for o in range(1, R):
        greet((me, flip(k, o)))
    get_idx = local(indices_h, indices, 0)
    get_len = local(lengths_h, bag_lengths, 1)

    @pl.when(core == 0)
    def follower():
        later = [local(top_fourth, w4.at[k], 2), local(top_last_h, top_last, 3)]
        get_idx.wait()
        get_len.wait()
        pair_idx[...] = own_tile()
        pl.semaphore_wait(barrier, R - 1)
        up = (me, mate)
        send(pair_idx, pair_idx, S_IDX, R_IDX, up)
        send(dense_h, dense.at[k], S_DENSE, R_DENSE, up)
        for o in range(1, X):
            lead = (me, flip(k, 2 * o + 1))
            send(dense_h, dense.at[k], S_DENSE, R_DENSE, lead)
            send(top_first, w1.at[k], S_W1, R_W1, lead)
            send(strip(o), w3.at[k], S_W3, R_W3, lead)
            send(top_fourth, w4.at[k], S_OWN, R_ACROSS + 2 * o, (me, flip(k, 2 * o)))
        send(top_first, w1.at[k], S_W1, R_W1, up)
        send(top_second, w2.at[0], S_W2, R_W2, up)
        send(strip(0), w3.at[k], S_W3, R_W3, up)
        send(top_fourth, w4.at[k], S_OWN, R_DOWN, up)
        if X > 1:
            arrive(w3.at[pl.ds(0, X - 1)], R_W3)
        for o in range(1, X):
            send(w3.at[o - 1], w3.at[mate], S_W3, R_W3, (me, flip(k, 2 * o + 1)))
        arrive(w4.at[mate], R_ACROSS)
        for o in range(1, X):
            send(w4.at[mate], w4.at[mate], S_FORWARD, R_ACROSS + 2 * o + 1, (me, flip(k, 2 * o)))
        for h in range(2):
            for o in range(1, X):
                block = w4.at[flip(k, 2 * o + h)]
                arrive(block, R_ACROSS + 2 * o + h)
                send(block, block, S_FORWARD, R_DOWN, up)
        for copy in later:
            copy.wait()
        last_column()
        arrive(recv_third, R_E4)
        finish()
        sent(pair_idx, S_IDX)
        sent(w2.at[0], S_W2)
        sent_blocks(dense, X, S_DENSE)
        sent_blocks(w1, X, S_W1)
        sent_blocks(w3, 2 * X - 1, S_W3)
        sent_blocks(w4, X, S_OWN)
        sent_blocks(w4, 3 * (X - 1), S_FORWARD)

    @pl.when(core == 1)
    def leader():
        for d in range(1, D):
            greet((flip(me, d), k))
        get_dense = local(dense_h, dense.at[k], 2)
        get_bottom = [
            local(bottom_first_h, bottom_first, 3),
            local(bottom_second_h, bottom_second, 4),
            local(bottom_third_h, bottom_third, 5),
        ]
        get_table = local(tables, table_v, 6)
        get_idx.wait()
        get_len.wait()
        later = [local(top_second, w2.at[1], 0), local(top_first, w1.at[k], 1)]
        mine = own_tile()
        pl.semaphore_wait(barrier, D - 1 + R - 1)
        arrive(pair_idx, R_IDX)
        out_idx[:, :HOT, :] = jnp.maximum(mine, pair_idx[...])

        for d in reversed(range(1, D)):
            peer = flip(me, d)
            send(
                out_idx.at[peer // per_table],
                recv_idx.at[me],
                S_E1,
                R_E1A if d < low else R_E1B,
                (peer, k),
            )
        recv_idx[me] = out_idx[me // per_table]
        for o in range(1, X):
            lead = (me, flip(k, 2 * o))
            send(dense_h, dense.at[k], S_DENSE, R_DENSE, lead)
            send(top_first, w1.at[k], S_W1, R_W1, lead)
            send(strip(o), w3.at[o - 1], S_W3, R_W3, (me, mate))
        send(top_fourth, w4.at[k], S_OWN, R_ACROSS, (me, mate))

        get_table.wait()
        table_t[...] = table_v[...].T

        offset = (me % per_table) * rows
        sub = lax.broadcasted_iota(jnp.int32, (PACK, LANES), 0)
        zero = jnp.zeros((PACK, LANES), BF16)

        def lookup(g):
            base = group * g
            entry = recv_idx[base, :HOT, :]
            for i in range(1, group):
                entry = jnp.maximum(entry, recv_idx[base + i, :HOT, :])
            codes, counts = [], []
            for s in range(HOT):
                row = jnp.broadcast_to(entry[s : s + 1, :], (PACK, LANES))
                spot = (row & (SPAN - 1)) - offset
                hit = jnp.logical_and((spot & (PACK - 1)) == sub, row >= 0)
                codes.append(jnp.where(hit, spot >> SHIFT, -1).astype(F32).astype(BF16))
                counts.append((row // SPAN).astype(F32).astype(BF16))
            partial = jnp.zeros((E, LANES), F32)
            for c in range(rows // CHUNK):
                chunk = []
                for n in range(c * CHUNK // PACK, (c + 1) * CHUNK // PACK):
                    total = zero
                    for code, count in zip(codes, counts):
                        total = jnp.where(code == jnp.asarray(n, BF16), count, total)
                    chunk.append(total)
                partial = partial + dot(
                    table_t[:, c * CHUNK : (c + 1) * CHUNK], jnp.concatenate(chunk, axis=0)
                )
            part[pl.ds(base, group)] = partial.T.reshape(group, 2 * B, E)

        def run(base, count):
            if count == group:
                lookup(base // group)
            else:
                pl.loop(0, count // group)(lambda g: lookup(base // group + g))

        def back(peer, to, rsem):
            send(part.at[peer], recv_pool.at[x * D + me], S_E2, rsem, (peer, to))

        def second_send(d):
            peer = flip(me, d)

            @pl.when(peer < early)
            def crossing():
                for o in range(1, X):
                    back(peer, flip(k, 2 * o), R_E2X)

            if d:

                @pl.when(peer >= early)
                def straight():
                    back(peer, k, R_E2)

        def second_send_late(d):
            peer = flip(me, d)

            @pl.when(peer < early)
            def straight():
                back(peer, k, R_E2)

        arrive(recv_idx.at[pl.ds(0, low - 1)], R_E1A)
        run(me // low * low, low)
        for d in reversed(range(low)):
            second_send(d)
        arrive(recv_idx.at[pl.ds(0, low)], R_E1B)
        run((1 - me // low) * low, low)
        for d in reversed(range(low, high)):
            second_send(d)
        recv_pool[x * D + me] = part[me]
        get_dense.wait()
        for copy in get_bottom:
            copy.wait()
        later += [
            local(strip(0), w3.at[k], 2),
            local(top_fourth, w4.at[k], 3),
            local(top_last_h, top_last, 4),
        ]
        arrive(dense.at[pl.ds(0, R - 1)], R_DENSE)
        arrive(w1.at[pl.ds(0, R - 1)], R_W1)
        lower = relu_round(dot(dense[...].reshape(R * B, -1), bottom_first[...]))
        middle = relu_round(dot(lower, bottom_second[...]))
        bottom_out = jnp.maximum(dot(middle, bottom_third[...]), 0.0)
        for d in reversed(range(1, D)):
            second_send_late(d)
        for copy in later:
            copy.wait()
        last_column()
        bottom[...] = bottom_out.reshape(X, 2 * B, E)
        bottom_in = bottom_out.astype(BF16)
        n1, n2 = w1.shape[2], w2.shape[2]
        for n in range(R):
            first[:, :, n * n1 : (n + 1) * n1] = dot(bottom_in, w1[n, :E, :]).reshape(
                X, 2 * B, n1
            )
        n3 = w3.shape[2]
        lane = lax.broadcasted_iota(jnp.int32, (2 * B, E), 1)

        def interact(y):
            features = [bottom[y]]
            for t in range(TAB):
                pooled = recv_pool[y * D + t * per_table]
                for i in range(1, per_table):
                    pooled = pooled + recv_pool[y * D + t * per_table + i]
                features.append(pooled)
            dots = jnp.zeros((2 * B, E), F32)
            p = 0
            for i in range(TAB + 1):
                for j in range(i + 1, TAB + 1):
                    value = jnp.sum(features[i] * features[j], axis=1, keepdims=True)
                    dots = jnp.where(lane == p, value, dots)
                    p += 1
            recv_dots[y] = dots.astype(BF16)

        def top(y):
            dots = recv_dots[y][:, : TAB * (TAB + 1) // 2]
            for n in range(R):
                act1[:, n * n1 : (n + 1) * n1] = relu_round(
                    first[y, :, n * n1 : (n + 1) * n1] + dot(dots, w1[n, E:, :])
                )
            act2 = jnp.concatenate([relu_round(dot(act1[...], w2[j])) for j in range(2)], axis=1)
            for n in range(R):
                third[pl.ds(2 * y, 2), :, n * n3 : (n + 1) * n3] = dot(act2, w3[n]).reshape(
                    2, B, n3
                )

        def weights():
            arrive(w2.at[0], R_W2)
            arrive(w3.at[pl.ds(0, R - 1)], R_W3)

        def others():
            for o in range(1, X):
                top(flip(x, o))
                for h in range(2):
                    to = flip(k, 2 * o + 1 - h)
                    send(third.at[to], recv_third.at[x], S_E4, R_E4, (me, to))

        def own():
            top(x)
            send(third.at[mate], recv_third.at[x], S_E4, R_E4, (me, mate))
            recv_third[x] = third[k]

        @pl.when(me < early)
        def ahead():
            if X > 1:
                arrive(recv_pool.at[pl.ds(0, (X - 1) * D)], R_E2X)
            for o in range(1, X):
                interact(flip(x, o))
            weights()
            others()
            arrive(recv_pool.at[pl.ds(0, D - 1)], R_E2)
            interact(x)
            own()

        @pl.when(me >= early)
        def behind():
            arrive(recv_pool.at[pl.ds(0, D - 1)], R_E2)
            interact(x)
            for o in range(1, X):
                send(recv_dots.at[x], recv_dots.at[x], S_E3, R_E3, (me, flip(k, 2 * o)))
            weights()
            own()
            if X > 1:
                arrive(recv_dots.at[pl.ds(0, X - 1)], R_E3)
            others()

        arrive(w4.at[pl.ds(0, R - 1)], R_DOWN)
        if X > 1:
            arrive(recv_third.at[pl.ds(0, X - 1)], R_E4)
        finish()
        sent(recv_idx.at[pl.ds(0, D - 1)], S_E1)
        sent_blocks(recv_pool, D - 1 + early * (X - 1), S_E2)
        sent(w4.at[k], S_OWN)
        sent(third.at[pl.ds(0, R - 1)], S_E4)
        if X > 1:
            sent_blocks(dense, X - 1, S_DENSE)
            sent_blocks(w1, X - 1, S_W1)
            sent_blocks(w3, X - 1, S_W3)

            @pl.when(me >= early)
            def sent_dots():
                sent(recv_dots.at[pl.ds(0, X - 1)], S_E3)


def body(*args):
    (tables, indices, bag_lengths, dense, b1, b2, b3, t1, t2, t3, t4, last) = args
    D = lax.axis_size("rows")
    R = lax.axis_size("rep")
    B = indices.shape[0]
    indices = jnp.transpose(indices, (1, 2, 0))
    bag_lengths = jnp.transpose(bag_lengths)
    t4 = jnp.transpose(t4)
    rows, E = tables.shape
    X = R // 2
    hbm = pl.BlockSpec(memory_space=pl.ANY)
    tile = pltpu.VMEM((TAB, HOT, LANES), jnp.int32)
    result = pl.pallas_call(
        functools.partial(kernel, D, R),
        out_shape=pltpu.VMEM((B,), F32),
        in_specs=[hbm] * 12,
        out_specs=pl.BlockSpec(memory_space=pltpu.VMEM),
        scratch_shapes=[
            pltpu.VMEM(indices.shape, jnp.int32),
            pltpu.VMEM(bag_lengths.shape, jnp.int32),
            pltpu.VMEM((R,) + dense.shape, BF16),
            pltpu.VMEM(b1.shape, BF16),
            pltpu.VMEM(b2.shape, BF16),
            pltpu.VMEM(b3.shape, BF16),
            pltpu.VMEM(last.shape, BF16),
            pltpu.VMEM((last.shape[0], B), F32),
            pltpu.VMEM((rows, E), BF16),
            pltpu.VMEM((E, rows), BF16),
            pltpu.VMEM((R,) + t1.shape, BF16),
            pltpu.VMEM((2,) + t2.shape, BF16),
            pltpu.VMEM((R, 2 * t2.shape[1], t3.shape[1]), BF16),
            pltpu.VMEM((R,) + t4.shape, BF16),
            tile,
            tile,
            pltpu.VMEM((TAB, HOT, LANES), jnp.int32),
            pltpu.VMEM((D, HOT, LANES), jnp.int32),
            pltpu.VMEM((D, 2 * B, E), F32),
            pltpu.VMEM((X * D, 2 * B, E), F32),
            pltpu.VMEM((X, 2 * B, E), BF16),
            pltpu.VMEM((X, 2 * B, E), F32),
            pltpu.VMEM((X, 2 * B, R * t1.shape[1]), F32),
            pltpu.VMEM((2 * B, R * t1.shape[1]), BF16),
            pltpu.VMEM((R, B, R * t3.shape[1]), F32),
            pltpu.VMEM((X, B, R * t3.shape[1]), F32),
            pltpu.SemaphoreType.DMA((max(27, R_ACROSS + R),)),
        ],
        compiler_params=pltpu.CompilerParams(collective_id=0, has_side_effects=True),
    )(tables, indices, bag_lengths, dense, b1, b2, b3, t1, t2, t3, t4, last)
    return result


def solution(mesh):
    placed = (
        P("rows", None),
        P(("rows", "rep"), None, None),
        P(("rows", "rep"), None),
        P(("rows", "rep"), None),
        P(),
        P(),
        P(),
        P(None, "rep"),
        P(None, "rep"),
        P(None, "rep"),
        P(None, "rep"),
        P(),
    )
    return jax.shard_map(
        body, mesh=mesh, in_specs=placed, out_specs=P(("rows", "rep")), check_vma=False
    )
```

```python
import functools

import jax
import jax.numpy as jnp
from jax import lax
from jax.experimental import pallas as pl
from jax.experimental.pallas import tpu as pltpu
from jax.sharding import PartitionSpec as P

TAB = 8
HOT = 8
LANES = 128
PACK = 16
SHIFT = 4
CHUNK = 256
EARLY = 8
SPAN = 65536
S_DENSE, S_W1, S_W3, S_OWN, S_E4, R_IDX, R_DENSE, R_W1, R_W2, R_W3, R_E4, R_DOWN = range(7, 19)
S_E1, S_E2, S_E3, R_E1, R_E1_LATE, R_E2, R_E2X, R_E3 = range(19, 27)
S_IDX, S_W2, S_FORWARD, R_ACROSS = range(19, 23)
MESH = pl.DeviceIdType.MESH
BF16 = jnp.bfloat16
F32 = jnp.float32


def flip(k, offset):
    bit = 1
    while bit <= offset:
        if offset & bit:
            k = k + bit - 2 * bit * ((k // bit) % 2)
        bit *= 2
    return k


def dot(a, b):
    return jnp.dot(a, b, preferred_element_type=F32)


def dot_t(a, b):
    return lax.dot_general(a, b, (((1,), (1,)), ((), ())), preferred_element_type=F32)


def relu_round(x):
    return jnp.maximum(x, 0.0).astype(BF16)


def kernel(
    D,
    R,
    tables,
    indices_h,
    lengths_h,
    dense_h,
    bottom_first_h,
    bottom_second_h,
    bottom_third_h,
    top_first,
    top_second,
    top_third,
    top_fourth,
    top_last_h,
    out,
    indices,
    bag_lengths,
    dense,
    bottom_first,
    bottom_second,
    bottom_third,
    top_last,
    last,
    table_v,
    table_t,
    w1,
    w2,
    w3,
    w4,
    own_idx,
    pair_idx,
    out_idx,
    recv_idx,
    part,
    recv_pool,
    recv_dots,
    bottom,
    first,
    act1,
    third,
    recv_third,
    sem,
):
    B = indices.shape[2]
    rows, E = tables.shape
    X = R // 2
    group = LANES // (2 * B)
    per_table = D // TAB
    me = lax.axis_index("rows")
    k = lax.axis_index("rep")
    core = k % 2
    x = k // 2
    mate = flip(k, 1)
    low, high = D // 2, D
    early = max(D // EARLY, 1)

    barrier = pltpu.get_barrier_semaphore()

    def greet(device):
        pl.semaphore_signal(barrier, inc=1, device_id=device, device_id_type=MESH)

    def local(src, dst, i):
        copy = pltpu.make_async_copy(src, dst, sem.at[i])
        copy.start()
        return copy

    def remote(src, dst, ssem, rsem, device):
        return pltpu.make_async_remote_copy(
            src_ref=src,
            dst_ref=dst,
            send_sem=sem.at[ssem],
            recv_sem=sem.at[rsem],
            device_id=device,
            device_id_type=MESH,
        )

    def send(src, dst, ssem, rsem, device):
        remote(src, dst, ssem, rsem, device).start()

    def arrive(dst, rsem):
        remote(dst, dst, rsem, rsem, (me, mate)).wait_recv()

    def sent(src, ssem):
        remote(src, src, ssem, ssem, (me, mate)).wait_send()

    def sent_blocks(stack, count, ssem):
        while count:
            now = min(count, stack.shape[0])
            sent(stack.at[pl.ds(0, now)], ssem)
            count -= now

    def own_tile():
        lens = bag_lengths[...].reshape(TAB, 1, B)
        slot = lax.broadcasted_iota(jnp.int32, (TAB, HOT, B), 1)
        own_idx[...] = jnp.full(own_idx.shape, -1, jnp.int32)
        own_idx[:, :, :B] = jnp.where(slot < lens, indices[...], -1)
        place = B * (2 * (me % group) + core)
        slot = lax.broadcasted_iota(jnp.int32, (HOT, LANES), 0)
        tiles = []
        for t in range(TAB):
            entry = own_idx[t]
            many = jnp.ones(entry.shape, jnp.int32)
            again = entry < 0
            for r in range(1, HOT):
                other = pltpu.roll(entry, r, 0)
                same = entry == other
                many = many + jnp.where(same, 1, 0)
                again = jnp.logical_or(again, jnp.logical_and(same, slot >= r))
            entry = jnp.where(again, -1, entry + many * SPAN)
            tiles.append(pltpu.roll(entry, place, 1))
        return jnp.stack(tiles)

    deep = w3.shape[1]

    def strip(o):
        return top_third.at[pl.ds(pl.multiple_of(flip(x, o) * deep, deep), deep)]

    def finish():
        total = recv_third[0]
        for n in range(1, X):
            total = total + recv_third[n]
        fourth_in = relu_round(total)
        last_in = relu_round(dot_t(w4[...].reshape(last.shape[0], -1), fourth_in))
        out[...] = jnp.sum(last_in.astype(F32) * last[...], axis=0)

    def last_column():
        row = top_last[...].reshape(1, -1).astype(F32)
        last[...] = jnp.broadcast_to(row, (B, row.shape[1])).T

    for o in range(1, R):
        greet((me, flip(k, o)))
    get_idx = local(indices_h, indices, 0)
    get_len = local(lengths_h, bag_lengths, 1)

    @pl.when(core == 0)
    def follower():
        later = [local(top_fourth, w4.at[k], 2), local(top_last_h, top_last, 3)]
        get_idx.wait()
        get_len.wait()
        pair_idx[...] = own_tile()
        pl.semaphore_wait(barrier, R - 1)
        up = (me, mate)
        send(pair_idx, pair_idx, S_IDX, R_IDX, up)
        send(dense_h, dense.at[k], S_DENSE, R_DENSE, up)
        for o in range(1, X):
            lead = (me, flip(k, 2 * o + 1))
            send(dense_h, dense.at[k], S_DENSE, R_DENSE, lead)
            send(top_first, w1.at[k], S_W1, R_W1, lead)
            send(strip(o), w3.at[k], S_W3, R_W3, lead)
            send(top_fourth, w4.at[k], S_OWN, R_ACROSS + 2 * o, (me, flip(k, 2 * o)))
        send(top_first, w1.at[k], S_W1, R_W1, up)
        send(top_second, w2.at[0], S_W2, R_W2, up)
        send(strip(0), w3.at[k], S_W3, R_W3, up)
        send(top_fourth, w4.at[k], S_OWN, R_DOWN, up)
        if X > 1:
            arrive(w3.at[pl.ds(0, X - 1)], R_W3)
        for o in range(1, X):
            send(w3.at[o - 1], w3.at[mate], S_W3, R_W3, (me, flip(k, 2 * o + 1)))
        arrive(w4.at[mate], R_ACROSS)
        for o in range(1, X):
            send(w4.at[mate], w4.at[mate], S_FORWARD, R_ACROSS + 2 * o + 1, (me, flip(k, 2 * o)))
        for h in range(2):
            for o in range(1, X):
                block = w4.at[flip(k, 2 * o + h)]
                arrive(block, R_ACROSS + 2 * o + h)
                send(block, block, S_FORWARD, R_DOWN, up)
        for copy in later:
            copy.wait()
        last_column()
        arrive(recv_third, R_E4)
        finish()
        sent(pair_idx, S_IDX)
        sent(w2.at[0], S_W2)
        sent_blocks(dense, X, S_DENSE)
        sent_blocks(w1, X, S_W1)
        sent_blocks(w3, 2 * X - 1, S_W3)
        sent_blocks(w4, X, S_OWN)
        sent_blocks(w4, 3 * (X - 1), S_FORWARD)

    @pl.when(core == 1)
    def leader():
        for d in range(1, D):
            greet((flip(me, d), k))
        get_dense = local(dense_h, dense.at[k], 2)
        get_bottom = [
            local(bottom_first_h, bottom_first, 3),
            local(bottom_second_h, bottom_second, 4),
            local(bottom_third_h, bottom_third, 5),
        ]
        get_table = local(tables, table_v, 6)
        get_idx.wait()
        get_len.wait()
        later = [local(top_second, w2.at[1], 0), local(top_first, w1.at[k], 1)]
        mine = own_tile()
        pl.semaphore_wait(barrier, D - 1 + R - 1)
        arrive(pair_idx, R_IDX)
        out_idx[:, :HOT, :] = jnp.maximum(mine, pair_idx[...])

        for d in reversed(range(1, D)):
            peer = flip(me, d)
            send(
                out_idx.at[peer // per_table],
                recv_idx.at[me],
                S_E1,
                R_E1 + me // low,
                (peer, k),
            )
        recv_idx[me] = out_idx[me // per_table]
        for o in range(1, X):
            lead = (me, flip(k, 2 * o))
            send(dense_h, dense.at[k], S_DENSE, R_DENSE, lead)
            send(top_first, w1.at[k], S_W1, R_W1, lead)
            send(strip(o), w3.at[o - 1], S_W3, R_W3, (me, mate))
        send(top_fourth, w4.at[k], S_OWN, R_ACROSS, (me, mate))

        get_table.wait()
        table_t[...] = table_v[...].T

        offset = (me % per_table) * rows
        sub = lax.broadcasted_iota(jnp.int32, (PACK, LANES), 0)
        zero = jnp.zeros((PACK, LANES), BF16)

        def lookup(g):
            base = group * g
            entry = recv_idx[base, :HOT, :]
            for i in range(1, group):
                entry = jnp.maximum(entry, recv_idx[base + i, :HOT, :])
            codes, counts = [], []
            for s in range(HOT):
                row = jnp.broadcast_to(entry[s : s + 1, :], (PACK, LANES))
                spot = (row & (SPAN - 1)) - offset
                hit = jnp.logical_and((spot & (PACK - 1)) == sub, row >= 0)
                codes.append(jnp.where(hit, spot >> SHIFT, -1).astype(F32).astype(BF16))
                counts.append((row // SPAN).astype(F32).astype(BF16))
            partial = jnp.zeros((E, LANES), F32)
            for c in range(rows // CHUNK):
                chunk = []
                for n in range(c * CHUNK // PACK, (c + 1) * CHUNK // PACK):
                    total = zero
                    for code, count in zip(codes, counts):
                        total = jnp.where(code == jnp.asarray(n, BF16), count, total)
                    chunk.append(total)
                partial = partial + dot(
                    table_t[:, c * CHUNK : (c + 1) * CHUNK], jnp.concatenate(chunk, axis=0)
                )
            part[pl.ds(base, group)] = partial.T.reshape(group, 2 * B, E)

        def run(base, count):
            if count == group:
                lookup(base // group)
            else:
                pl.loop(0, count // group)(lambda g: lookup(base // group + g))

        def back(peer, to, rsem):
            send(part.at[peer], recv_pool.at[x * D + me], S_E2, rsem, (peer, to))

        def second_send(r):
            if r < early:
                for o in range(1, X):
                    back(r, flip(k, 2 * o), R_E2X)
            else:
                second_send_straight(r)

        def second_send_straight(r):
            @pl.when(me != r)
            def straight():
                back(r, k, R_E2)

        for half in range(2):

            @pl.when(me // low == half)
            def from_own_half():
                arrive(recv_idx.at[pl.ds(0, low - 1)], R_E1 + half)

            @pl.when(me // low != half)
            def from_other_half():
                arrive(recv_idx.at[pl.ds(0, low)], R_E1 + half)

            run(half * low, low)
            for r in range(half * low, (half + 1) * low):
                second_send(r)
        recv_pool[x * D + me] = part[me]
        get_dense.wait()
        for copy in get_bottom:
            copy.wait()
        later += [
            local(strip(0), w3.at[k], 2),
            local(top_fourth, w4.at[k], 3),
            local(top_last_h, top_last, 4),
        ]
        arrive(dense.at[pl.ds(0, R - 1)], R_DENSE)
        arrive(w1.at[pl.ds(0, R - 1)], R_W1)
        lower = relu_round(dot(dense[...].reshape(R * B, -1), bottom_first[...]))
        middle = relu_round(dot(lower, bottom_second[...]))
        bottom_out = jnp.maximum(dot(middle, bottom_third[...]), 0.0)
        for r in range(early):
            second_send_straight(r)
        for copy in later:
            copy.wait()
        last_column()
        bottom[...] = bottom_out.reshape(X, 2 * B, E)
        bottom_in = bottom_out.astype(BF16)
        n1, n2 = w1.shape[2], w2.shape[2]
        for n in range(R):
            first[:, :, n * n1 : (n + 1) * n1] = dot(bottom_in, w1[n, :E, :]).reshape(
                X, 2 * B, n1
            )
        n3 = w3.shape[2]
        lane = lax.broadcasted_iota(jnp.int32, (2 * B, E), 1)

        def interact(y):
            features = [bottom[y]]
            for t in range(TAB):
                pooled = recv_pool[y * D + t * per_table]
                for i in range(1, per_table):
                    pooled = pooled + recv_pool[y * D + t * per_table + i]
                features.append(pooled)
            dots = jnp.zeros((2 * B, E), F32)
            p = 0
            for i in range(TAB + 1):
                for j in range(i + 1, TAB + 1):
                    value = jnp.sum(features[i] * features[j], axis=1, keepdims=True)
                    dots = jnp.where(lane == p, value, dots)
                    p += 1
            recv_dots[y] = dots.astype(BF16)

        def top(y):
            dots = recv_dots[y][:, : TAB * (TAB + 1) // 2]
            for n in range(R):
                act1[:, n * n1 : (n + 1) * n1] = relu_round(
                    first[y, :, n * n1 : (n + 1) * n1] + dot(dots, w1[n, E:, :])
                )
            act2 = jnp.concatenate([relu_round(dot(act1[...], w2[j])) for j in range(2)], axis=1)
            for n in range(R):
                third[pl.ds(2 * y, 2), :, n * n3 : (n + 1) * n3] = dot(act2, w3[n]).reshape(
                    2, B, n3
                )

        def weights():
            arrive(w2.at[0], R_W2)
            arrive(w3.at[pl.ds(0, R - 1)], R_W3)

        def others():
            for o in range(1, X):
                top(flip(x, o))
                for h in range(2):
                    to = flip(k, 2 * o + 1 - h)
                    send(third.at[to], recv_third.at[x], S_E4, R_E4, (me, to))

        def own():
            top(x)
            send(third.at[mate], recv_third.at[x], S_E4, R_E4, (me, mate))
            recv_third[x] = third[k]

        @pl.when(me < early)
        def ahead():
            if X > 1:
                arrive(recv_pool.at[pl.ds(0, (X - 1) * D)], R_E2X)
            for o in range(1, X):
                interact(flip(x, o))
            weights()
            others()
            arrive(recv_pool.at[pl.ds(0, D - 1)], R_E2)
            interact(x)
            own()

        @pl.when(me >= early)
        def behind():
            arrive(recv_pool.at[pl.ds(0, D - 1)], R_E2)
            interact(x)
            for o in range(1, X):
                send(recv_dots.at[x], recv_dots.at[x], S_E3, R_E3, (me, flip(k, 2 * o)))
            weights()
            own()
            if X > 1:
                arrive(recv_dots.at[pl.ds(0, X - 1)], R_E3)
            others()

        arrive(w4.at[pl.ds(0, R - 1)], R_DOWN)
        if X > 1:
            arrive(recv_third.at[pl.ds(0, X - 1)], R_E4)
        finish()
        sent(recv_idx.at[pl.ds(0, D - 1)], S_E1)
        sent_blocks(recv_pool, D - 1 + early * (X - 1), S_E2)
        sent(w4.at[k], S_OWN)
        sent(third.at[pl.ds(0, R - 1)], S_E4)
        if X > 1:
            sent_blocks(dense, X - 1, S_DENSE)
            sent_blocks(w1, X - 1, S_W1)
            sent_blocks(w3, X - 1, S_W3)

            @pl.when(me >= early)
            def sent_dots():
                sent(recv_dots.at[pl.ds(0, X - 1)], S_E3)


def body(*args):
    (tables, indices, bag_lengths, dense, b1, b2, b3, t1, t2, t3, t4, last) = args
    D = lax.axis_size("rows")
    R = lax.axis_size("rep")
    B = indices.shape[0]
    indices = jnp.transpose(indices, (1, 2, 0))
    bag_lengths = jnp.transpose(bag_lengths)
    t4 = jnp.transpose(t4)
    rows, E = tables.shape
    X = R // 2
    hbm = pl.BlockSpec(memory_space=pl.ANY)
    tile = pltpu.VMEM((TAB, HOT, LANES), jnp.int32)
    result = pl.pallas_call(
        functools.partial(kernel, D, R),
        out_shape=pltpu.VMEM((B,), F32),
        in_specs=[hbm] * 12,
        out_specs=pl.BlockSpec(memory_space=pltpu.VMEM),
        scratch_shapes=[
            pltpu.VMEM(indices.shape, jnp.int32),
            pltpu.VMEM(bag_lengths.shape, jnp.int32),
            pltpu.VMEM((R,) + dense.shape, BF16),
            pltpu.VMEM(b1.shape, BF16),
            pltpu.VMEM(b2.shape, BF16),
            pltpu.VMEM(b3.shape, BF16),
            pltpu.VMEM(last.shape, BF16),
            pltpu.VMEM((last.shape[0], B), F32),
            pltpu.VMEM((rows, E), BF16),
            pltpu.VMEM((E, rows), BF16),
            pltpu.VMEM((R,) + t1.shape, BF16),
            pltpu.VMEM((2,) + t2.shape, BF16),
            pltpu.VMEM((R, 2 * t2.shape[1], t3.shape[1]), BF16),
            pltpu.VMEM((R,) + t4.shape, BF16),
            tile,
            tile,
            pltpu.VMEM((TAB, HOT, LANES), jnp.int32),
            pltpu.VMEM((D, HOT, LANES), jnp.int32),
            pltpu.VMEM((D, 2 * B, E), F32),
            pltpu.VMEM((X * D, 2 * B, E), F32),
            pltpu.VMEM((X, 2 * B, E), BF16),
            pltpu.VMEM((X, 2 * B, E), F32),
            pltpu.VMEM((X, 2 * B, R * t1.shape[1]), F32),
            pltpu.VMEM((2 * B, R * t1.shape[1]), BF16),
            pltpu.VMEM((R, B, R * t3.shape[1]), F32),
            pltpu.VMEM((X, B, R * t3.shape[1]), F32),
            pltpu.SemaphoreType.DMA((max(27, R_ACROSS + R),)),
        ],
        compiler_params=pltpu.CompilerParams(collective_id=0, has_side_effects=True),
    )(tables, indices, bag_lengths, dense, b1, b2, b3, t1, t2, t3, t4, last)
    return result


def solution(mesh):
    placed = (
        P("rows", None),
        P(("rows", "rep"), None, None),
        P(("rows", "rep"), None),
        P(("rows", "rep"), None),
        P(),
        P(),
        P(),
        P(None, "rep"),
        P(None, "rep"),
        P(None, "rep"),
        P(None, "rep"),
        P(),
    )
    return jax.shard_map(
        body, mesh=mesh, in_specs=placed, out_specs=P(("rows", "rep")), check_vma=False
    )
```

```python
import functools

import jax
import jax.numpy as jnp
from jax import lax
from jax.experimental import pallas as pl
from jax.experimental.pallas import tpu as pltpu
from jax.sharding import PartitionSpec as P

TAB = 8
HOT = 8
LANES = 128
PACK = 16
SHIFT = 4
CHUNK = 512
EARLY = 8
SPAN = 65536
S_DENSE, S_W1, S_W3, S_OWN, S_E4, R_IDX, R_DENSE, R_W1, R_W2, R_W3, R_E4, R_DOWN = range(7, 19)
S_E1, S_E2, S_E3, R_E1, R_E1_LATE, R_E2, R_E2X, R_E2Y, R_E3 = range(19, 28)
S_IDX, S_W2, S_FORWARD, R_ACROSS = range(19, 23)
MESH = pl.DeviceIdType.MESH
BF16 = jnp.bfloat16
F32 = jnp.float32


def flip(k, offset):
    bit = 1
    while bit <= offset:
        if offset & bit:
            k = k + bit - 2 * bit * ((k // bit) % 2)
        bit *= 2
    return k


def dot(a, b):
    return jnp.dot(a, b, preferred_element_type=F32)


def dot_t(a, b):
    return lax.dot_general(a, b, (((1,), (1,)), ((), ())), preferred_element_type=F32)


def relu_round(x):
    return jnp.maximum(x, 0.0).astype(BF16)


def kernel(
    D,
    R,
    tables,
    indices_h,
    lengths_h,
    dense_h,
    bottom_first_h,
    bottom_second_h,
    bottom_third_h,
    top_first,
    top_second,
    top_third,
    top_fourth,
    top_last_h,
    out,
    indices,
    bag_lengths,
    dense,
    bottom_first,
    bottom_second,
    bottom_third,
    top_last,
    last,
    table_v,
    table_t,
    w1,
    w2,
    w3,
    w4,
    own_idx,
    pair_idx,
    out_idx,
    recv_idx,
    part,
    recv_pool,
    recv_dots,
    bottom,
    first,
    act1,
    third,
    recv_third,
    sem,
):
    B = indices.shape[2]
    rows, E = tables.shape
    X = R // 2
    group = LANES // (2 * B)
    per_table = D // TAB
    me = lax.axis_index("rows")
    k = lax.axis_index("rep")
    core = k % 2
    x = k // 2
    mate = flip(k, 1)
    low, high = D // 2, D
    early = max(D // EARLY, 1)

    barrier = pltpu.get_barrier_semaphore()

    def greet(device):
        pl.semaphore_signal(barrier, inc=1, device_id=device, device_id_type=MESH)

    def local(src, dst, i):
        copy = pltpu.make_async_copy(src, dst, sem.at[i])
        copy.start()
        return copy

    def remote(src, dst, ssem, rsem, device):
        return pltpu.make_async_remote_copy(
            src_ref=src,
            dst_ref=dst,
            send_sem=sem.at[ssem],
            recv_sem=sem.at[rsem],
            device_id=device,
            device_id_type=MESH,
        )

    def send(src, dst, ssem, rsem, device):
        remote(src, dst, ssem, rsem, device).start()

    def arrive(dst, rsem):
        remote(dst, dst, rsem, rsem, (me, mate)).wait_recv()

    def sent(src, ssem):
        remote(src, src, ssem, ssem, (me, mate)).wait_send()

    def sent_blocks(stack, count, ssem):
        while count:
            now = min(count, stack.shape[0])
            sent(stack.at[pl.ds(0, now)], ssem)
            count -= now

    def own_tile():
        lens = bag_lengths[...].reshape(TAB, 1, B)
        slot = lax.broadcasted_iota(jnp.int32, (TAB, HOT, B), 1)
        own_idx[...] = jnp.full(own_idx.shape, -1, jnp.int32)
        own_idx[:, :, :B] = jnp.where(slot < lens, indices[...], -1)
        place = B * (2 * (me % group) + core)
        slot = lax.broadcasted_iota(jnp.int32, (HOT, LANES), 0)
        tiles = []
        for t in range(TAB):
            entry = own_idx[t]
            many = jnp.ones(entry.shape, jnp.int32)
            again = entry < 0
            for r in range(1, HOT):
                other = pltpu.roll(entry, r, 0)
                same = entry == other
                many = many + jnp.where(same, 1, 0)
                again = jnp.logical_or(again, jnp.logical_and(same, slot >= r))
            entry = jnp.where(again, -1, entry + many * SPAN)
            tiles.append(pltpu.roll(entry, place, 1))
        return jnp.stack(tiles)

    deep = w3.shape[1]

    def strip(o):
        return top_third.at[pl.ds(pl.multiple_of(flip(x, o) * deep, deep), deep)]

    def finish():
        total = recv_third[0]
        for n in range(1, X):
            total = total + recv_third[n]
        fourth_in = relu_round(total)
        last_in = relu_round(dot_t(w4[...].reshape(last.shape[0], -1), fourth_in))
        out[...] = jnp.sum(last_in.astype(F32) * last[...], axis=0)

    def last_column():
        row = top_last[...].reshape(1, -1).astype(F32)
        last[...] = jnp.broadcast_to(row, (B, row.shape[1])).T

    for o in range(1, R):
        greet((me, flip(k, o)))
    get_idx = local(indices_h, indices, 0)
    get_len = local(lengths_h, bag_lengths, 1)

    @pl.when(core == 0)
    def follower():
        later = [local(top_fourth, w4.at[k], 2), local(top_last_h, top_last, 3)]
        get_idx.wait()
        get_len.wait()
        pair_idx[...] = own_tile()
        pl.semaphore_wait(barrier, R - 1)
        up = (me, mate)
        send(pair_idx, pair_idx, S_IDX, R_IDX, up)
        send(dense_h, dense.at[k], S_DENSE, R_DENSE, up)
        for o in range(1, X):
            lead = (me, flip(k, 2 * o + 1))
            send(dense_h, dense.at[k], S_DENSE, R_DENSE, lead)
            send(top_first, w1.at[k], S_W1, R_W1, lead)
            send(strip(o), w3.at[k], S_W3, R_W3, lead)
            send(top_fourth, w4.at[k], S_OWN, R_ACROSS + 2 * o, (me, flip(k, 2 * o)))
        send(top_first, w1.at[k], S_W1, R_W1, up)
        send(top_second, w2.at[0], S_W2, R_W2, up)
        send(strip(0), w3.at[k], S_W3, R_W3, up)
        send(top_fourth, w4.at[k], S_OWN, R_DOWN, up)
        if X > 1:
            arrive(w3.at[pl.ds(0, X - 1)], R_W3)
        for o in range(1, X):
            send(w3.at[o - 1], w3.at[mate], S_W3, R_W3, (me, flip(k, 2 * o + 1)))
        arrive(w4.at[mate], R_ACROSS)
        for o in range(1, X):
            send(w4.at[mate], w4.at[mate], S_FORWARD, R_ACROSS + 2 * o + 1, (me, flip(k, 2 * o)))
        for h in range(2):
            for o in range(1, X):
                block = w4.at[flip(k, 2 * o + h)]
                arrive(block, R_ACROSS + 2 * o + h)
                send(block, block, S_FORWARD, R_DOWN, up)
        for copy in later:
            copy.wait()
        last_column()
        arrive(recv_third, R_E4)
        finish()
        sent(pair_idx, S_IDX)
        sent(w2.at[0], S_W2)
        sent_blocks(dense, X, S_DENSE)
        sent_blocks(w1, X, S_W1)
        sent_blocks(w3, 2 * X - 1, S_W3)
        sent_blocks(w4, X, S_OWN)
        sent_blocks(w4, 3 * (X - 1), S_FORWARD)

    @pl.when(core == 1)
    def leader():
        for d in range(1, D):
            greet((flip(me, d), k))
        get_dense = local(dense_h, dense.at[k], 2)
        get_bottom = [
            local(bottom_first_h, bottom_first, 3),
            local(bottom_second_h, bottom_second, 4),
            local(bottom_third_h, bottom_third, 5),
        ]
        get_table = local(tables, table_v, 6)
        get_idx.wait()
        get_len.wait()
        later = [local(top_second, w2.at[1], 0), local(top_first, w1.at[k], 1)]
        mine = own_tile()
        pl.semaphore_wait(barrier, D - 1 + R - 1)
        arrive(pair_idx, R_IDX)
        out_idx[:, :HOT, :] = jnp.maximum(mine, pair_idx[...])

        for d in reversed(range(1, D)):
            peer = flip(me, d)
            send(
                out_idx.at[peer // per_table],
                recv_idx.at[me],
                S_E1,
                R_E1 + me // low,
                (peer, k),
            )
        recv_idx[me] = out_idx[me // per_table]
        for o in range(1, X):
            lead = (me, flip(k, 2 * o))
            send(dense_h, dense.at[k], S_DENSE, R_DENSE, lead)
            send(top_first, w1.at[k], S_W1, R_W1, lead)
            send(strip(o), w3.at[o - 1], S_W3, R_W3, (me, mate))
        send(top_fourth, w4.at[k], S_OWN, R_ACROSS, (me, mate))

        get_table.wait()
        table_t[...] = table_v[...].T

        offset = (me % per_table) * rows
        sub = lax.broadcasted_iota(jnp.int32, (PACK, LANES), 0)
        zero = jnp.zeros((PACK, LANES), BF16)

        def lookup(g):
            base = group * g
            entry = recv_idx[base, :HOT, :]
            for i in range(1, group):
                entry = jnp.maximum(entry, recv_idx[base + i, :HOT, :])
            codes, counts = [], []
            for s in range(HOT):
                row = jnp.broadcast_to(entry[s : s + 1, :], (PACK, LANES))
                spot = (row & (SPAN - 1)) - offset
                hit = jnp.logical_and((spot & (PACK - 1)) == sub, row >= 0)
                codes.append(jnp.where(hit, spot >> SHIFT, -1).astype(F32).astype(BF16))
                counts.append((row // SPAN).astype(F32).astype(BF16))
            partial = jnp.zeros((E, LANES), F32)
            for c in range(rows // CHUNK):
                chunk = []
                for n in range(c * CHUNK // PACK, (c + 1) * CHUNK // PACK):
                    total = zero
                    for code, count in zip(codes, counts):
                        total = jnp.where(code == jnp.asarray(n, BF16), count, total)
                    chunk.append(total)
                partial = partial + dot(
                    table_t[:, c * CHUNK : (c + 1) * CHUNK], jnp.concatenate(chunk, axis=0)
                )
            part[pl.ds(base, group)] = partial.T.reshape(group, 2 * B, E)

        def run(base, count):
            if count == group:
                lookup(base // group)
            else:
                pl.loop(0, count // group)(lambda g: lookup(base // group + g))

        def back(peer, to, rsem):
            send(part.at[peer], recv_pool.at[x * D + me], S_E2, rsem, (peer, to))

        def second_send(r):
            if r < early:
                for o in range(1, X):
                    back(r, flip(k, 2 * o), R_E2X + (R_E2Y - R_E2X) * (me // low))

                @pl.when(x == 0)
                def at_once():
                    second_send_straight(r)

            else:
                second_send_straight(r)

        def second_send_straight(r):
            @pl.when(me != r)
            def straight():
                back(r, k, R_E2)

        for half in range(2):

            @pl.when(me // low == half)
            def from_own_half():
                arrive(recv_idx.at[pl.ds(0, low - 1)], R_E1 + half)

            @pl.when(me // low != half)
            def from_other_half():
                arrive(recv_idx.at[pl.ds(0, low)], R_E1 + half)

            run(half * low, low)
            for r in range(half * low, (half + 1) * low):
                second_send(r)
        recv_pool[x * D + me] = part[me]
        get_dense.wait()
        for copy in get_bottom:
            copy.wait()
        later += [
            local(strip(0), w3.at[k], 2),
            local(top_fourth, w4.at[k], 3),
            local(top_last_h, top_last, 4),
        ]
        arrive(dense.at[pl.ds(0, R - 1)], R_DENSE)
        arrive(w1.at[pl.ds(0, R - 1)], R_W1)
        lower = relu_round(dot(dense[...].reshape(R * B, -1), bottom_first[...]))
        middle = relu_round(dot(lower, bottom_second[...]))
        bottom_out = jnp.maximum(dot(middle, bottom_third[...]), 0.0)
        @pl.when(x > 0)
        def not_urgent():
            for r in range(early):
                second_send_straight(r)

        for copy in later:
            copy.wait()
        last_column()
        bottom[...] = bottom_out.reshape(X, 2 * B, E)
        bottom_in = bottom_out.astype(BF16)
        n1, n2 = w1.shape[2], w2.shape[2]
        for n in range(R):
            first[:, :, n * n1 : (n + 1) * n1] = dot(bottom_in, w1[n, :E, :]).reshape(
                X, 2 * B, n1
            )
        n3 = w3.shape[2]
        lane = lax.broadcasted_iota(jnp.int32, (2 * B, E), 1)

        def feature(y, t):
            pooled = recv_pool[y * D + t * per_table]
            for i in range(1, per_table):
                pooled = pooled + recv_pool[y * D + t * per_table + i]
            return pooled

        def pairs(y, features, dots, wanted):
            p = 0
            for i in range(TAB + 1):
                for j in range(i + 1, TAB + 1):
                    if wanted(j):
                        value = jnp.sum(features[i] * features[j], axis=1, keepdims=True)
                        dots = jnp.where(lane == p, value, dots)
                    p += 1
            return dots

        def interact(y, between=None):
            dots = jnp.zeros((2 * B, E), F32)
            features = [bottom[y]]
            if between is None:
                features += [feature(y, t) for t in range(TAB)]
                dots = pairs(y, features, dots, lambda j: True)
            else:
                features += [feature(y, t) for t in range(TAB // 2)]
                dots = pairs(y, features, dots, lambda j: j <= TAB // 2)
                between()
                features += [feature(y, t) for t in range(TAB // 2, TAB)]
                dots = pairs(y, features, dots, lambda j: j > TAB // 2)
            recv_dots[y] = dots.astype(BF16)

        def top(y):
            dots = recv_dots[y][:, : TAB * (TAB + 1) // 2]
            for n in range(R):
                act1[:, n * n1 : (n + 1) * n1] = relu_round(
                    first[y, :, n * n1 : (n + 1) * n1] + dot(dots, w1[n, E:, :])
                )
            act2 = jnp.concatenate([relu_round(dot(act1[...], w2[j])) for j in range(2)], axis=1)
            for n in range(R):
                third[pl.ds(2 * y, 2), :, n * n3 : (n + 1) * n3] = dot(act2, w3[n]).reshape(
                    2, B, n3
                )

        def weights():
            arrive(w2.at[0], R_W2)
            arrive(w3.at[pl.ds(0, R - 1)], R_W3)

        def others():
            for o in range(1, X):
                top(flip(x, o))
                for h in range(2):
                    to = flip(k, 2 * o + 1 - h)
                    send(third.at[to], recv_third.at[x], S_E4, R_E4, (me, to))

        def own():
            top(x)
            send(third.at[mate], recv_third.at[x], S_E4, R_E4, (me, mate))
            recv_third[x] = third[k]

        @pl.when(jnp.logical_and(me < early, x == 0))
        def foremost():
            arrive(recv_pool.at[pl.ds(0, D - 1)], R_E2)
            interact(x)
            weights()
            own()
            if X > 1:
                lower = pl.ds(0, (X - 1) * low)
                arrive(recv_pool.at[lower], R_E2X)
                if X == 2:
                    interact(flip(x, 1), lambda: arrive(recv_pool.at[lower], R_E2Y))
                else:
                    arrive(recv_pool.at[lower], R_E2Y)
                    for o in range(1, X):
                        interact(flip(x, o))
            others()

        @pl.when(jnp.logical_and(me < early, x > 0))
        def ahead():
            if X > 1:
                lower = pl.ds(0, (X - 1) * low)
                arrive(recv_pool.at[lower], R_E2X)
                if X == 2:
                    interact(flip(x, 1), lambda: arrive(recv_pool.at[lower], R_E2Y))
                else:
                    arrive(recv_pool.at[lower], R_E2Y)
                    for o in range(1, X):
                        interact(flip(x, o))
            weights()
            others()
            arrive(recv_pool.at[pl.ds(0, D - 1)], R_E2)
            interact(x)
            own()

        @pl.when(me >= early)
        def behind():
            arrive(recv_pool.at[pl.ds(0, D - 1)], R_E2)
            interact(x)
            for o in range(1, X):
                send(recv_dots.at[x], recv_dots.at[x], S_E3, R_E3, (me, flip(k, 2 * o)))
            weights()
            own()
            if X > 1:
                arrive(recv_dots.at[pl.ds(0, X - 1)], R_E3)
            others()

        arrive(w4.at[pl.ds(0, R - 1)], R_DOWN)
        if X > 1:
            arrive(recv_third.at[pl.ds(0, X - 1)], R_E4)
        finish()
        sent(recv_idx.at[pl.ds(0, D - 1)], S_E1)
        sent_blocks(recv_pool, D - 1 + early * (X - 1), S_E2)
        sent(w4.at[k], S_OWN)
        sent(third.at[pl.ds(0, R - 1)], S_E4)
        if X > 1:
            sent_blocks(dense, X - 1, S_DENSE)
            sent_blocks(w1, X - 1, S_W1)
            sent_blocks(w3, X - 1, S_W3)

            @pl.when(me >= early)
            def sent_dots():
                sent(recv_dots.at[pl.ds(0, X - 1)], S_E3)


def body(*args):
    (tables, indices, bag_lengths, dense, b1, b2, b3, t1, t2, t3, t4, last) = args
    D = lax.axis_size("rows")
    R = lax.axis_size("rep")
    B = indices.shape[0]
    indices = jnp.transpose(indices, (1, 2, 0))
    bag_lengths = jnp.transpose(bag_lengths)
    t4 = jnp.transpose(t4)
    rows, E = tables.shape
    X = R // 2
    hbm = pl.BlockSpec(memory_space=pl.ANY)
    tile = pltpu.VMEM((TAB, HOT, LANES), jnp.int32)
    result = pl.pallas_call(
        functools.partial(kernel, D, R),
        out_shape=pltpu.VMEM((B,), F32),
        in_specs=[hbm] * 12,
        out_specs=pl.BlockSpec(memory_space=pltpu.VMEM),
        scratch_shapes=[
            pltpu.VMEM(indices.shape, jnp.int32),
            pltpu.VMEM(bag_lengths.shape, jnp.int32),
            pltpu.VMEM((R,) + dense.shape, BF16),
            pltpu.VMEM(b1.shape, BF16),
            pltpu.VMEM(b2.shape, BF16),
            pltpu.VMEM(b3.shape, BF16),
            pltpu.VMEM(last.shape, BF16),
            pltpu.VMEM((last.shape[0], B), F32),
            pltpu.VMEM((rows, E), BF16),
            pltpu.VMEM((E, rows), BF16),
            pltpu.VMEM((R,) + t1.shape, BF16),
            pltpu.VMEM((2,) + t2.shape, BF16),
            pltpu.VMEM((R, 2 * t2.shape[1], t3.shape[1]), BF16),
            pltpu.VMEM((R,) + t4.shape, BF16),
            tile,
            tile,
            pltpu.VMEM((TAB, HOT, LANES), jnp.int32),
            pltpu.VMEM((D, HOT, LANES), jnp.int32),
            pltpu.VMEM((D, 2 * B, E), F32),
            pltpu.VMEM((X * D, 2 * B, E), F32),
            pltpu.VMEM((X, 2 * B, E), BF16),
            pltpu.VMEM((X, 2 * B, E), F32),
            pltpu.VMEM((X, 2 * B, R * t1.shape[1]), F32),
            pltpu.VMEM((2 * B, R * t1.shape[1]), BF16),
            pltpu.VMEM((R, B, R * t3.shape[1]), F32),
            pltpu.VMEM((X, B, R * t3.shape[1]), F32),
            pltpu.SemaphoreType.DMA((max(28, R_ACROSS + R),)),
        ],
        compiler_params=pltpu.CompilerParams(collective_id=0, has_side_effects=True),
    )(tables, indices, bag_lengths, dense, b1, b2, b3, t1, t2, t3, t4, last)
    return result


def solution(mesh):
    placed = (
        P("rows", None),
        P(("rows", "rep"), None, None),
        P(("rows", "rep"), None),
        P(("rows", "rep"), None),
        P(),
        P(),
        P(),
        P(None, "rep"),
        P(None, "rep"),
        P(None, "rep"),
        P(None, "rep"),
        P(),
    )
    return jax.shard_map(
        body, mesh=mesh, in_specs=placed, out_specs=P(("rows", "rep")), check_vma=False
    )
```

```python
import functools

import jax
import jax.numpy as jnp
from jax import lax
from jax.experimental import pallas as pl
from jax.experimental.pallas import tpu as pltpu
from jax.sharding import PartitionSpec as P

TAB = 8
HOT = 8
LANES = 128
PACK = 16
SHIFT = 4
CHUNK = 512
EARLY = 8
SPAN = 65536
S_DENSE, S_W1, S_W3, S_OWN, S_E4, R_IDX, R_DENSE, R_W1, R_W2, R_W3, R_E4, R_DOWN = range(7, 19)
S_E1, S_E2, S_E3, R_E1, R_E1_LATE, R_E2, R_E2X, R_E3 = range(19, 27)
S_IDX, S_W2, S_FORWARD, R_ACROSS = range(19, 23)
MESH = pl.DeviceIdType.MESH
BF16 = jnp.bfloat16
F32 = jnp.float32


def flip(k, offset):
    bit = 1
    while bit <= offset:
        if offset & bit:
            k = k + bit - 2 * bit * ((k // bit) % 2)
        bit *= 2
    return k


def dot(a, b):
    return jnp.dot(a, b, preferred_element_type=F32)


def dot_t(a, b):
    return lax.dot_general(a, b, (((1,), (1,)), ((), ())), preferred_element_type=F32)


def relu_round(x):
    return jnp.maximum(x, 0.0).astype(BF16)


def kernel(
    D,
    R,
    tables,
    indices_h,
    lengths_h,
    dense_h,
    bottom_first_h,
    bottom_second_h,
    bottom_third_h,
    top_first,
    top_second,
    top_third,
    top_fourth,
    top_last_h,
    out,
    indices,
    bag_lengths,
    dense,
    bottom_first,
    bottom_second,
    bottom_third,
    top_last,
    last,
    table_v,
    table_t,
    w1,
    w2,
    w3,
    w4,
    own_idx,
    pair_idx,
    out_idx,
    recv_idx,
    part,
    recv_pool,
    recv_dots,
    bottom,
    first,
    act1,
    third,
    recv_third,
    sem,
):
    B = indices.shape[2]
    rows, E = tables.shape
    X = R // 2
    group = LANES // (2 * B)
    per_table = D // TAB
    me = lax.axis_index("rows")
    k = lax.axis_index("rep")
    core = k % 2
    x = k // 2
    mate = flip(k, 1)
    low, high = D // 2, D
    early = max(D // EARLY, 1)

    barrier = pltpu.get_barrier_semaphore()

    def greet(device):
        pl.semaphore_signal(barrier, inc=1, device_id=device, device_id_type=MESH)

    def local(src, dst, i):
        copy = pltpu.make_async_copy(src, dst, sem.at[i])
        copy.start()
        return copy

    def remote(src, dst, ssem, rsem, device):
        return pltpu.make_async_remote_copy(
            src_ref=src,
            dst_ref=dst,
            send_sem=sem.at[ssem],
            recv_sem=sem.at[rsem],
            device_id=device,
            device_id_type=MESH,
        )

    def send(src, dst, ssem, rsem, device):
        remote(src, dst, ssem, rsem, device).start()

    def arrive(dst, rsem):
        remote(dst, dst, rsem, rsem, (me, mate)).wait_recv()

    def sent(src, ssem):
        remote(src, src, ssem, ssem, (me, mate)).wait_send()

    def sent_blocks(stack, count, ssem):
        while count:
            now = min(count, stack.shape[0])
            sent(stack.at[pl.ds(0, now)], ssem)
            count -= now

    def own_tile():
        lens = bag_lengths[...].reshape(TAB, 1, B)
        slot = lax.broadcasted_iota(jnp.int32, (TAB, HOT, B), 1)
        own_idx[...] = jnp.full(own_idx.shape, -1, jnp.int32)
        own_idx[:, :, :B] = jnp.where(slot < lens, indices[...], -1)
        place = B * (2 * (me % group) + core)
        slot = lax.broadcasted_iota(jnp.int32, (HOT, LANES), 0)
        tiles = []
        for t in range(TAB):
            entry = own_idx[t]
            many = jnp.ones(entry.shape, jnp.int32)
            again = entry < 0
            for r in range(1, HOT):
                other = pltpu.roll(entry, r, 0)
                same = entry == other
                many = many + jnp.where(same, 1, 0)
                again = jnp.logical_or(again, jnp.logical_and(same, slot >= r))
            entry = jnp.where(again, -1, entry + many * SPAN)
            tiles.append(pltpu.roll(entry, place, 1))
        return jnp.stack(tiles)

    deep = w3.shape[1]

    def strip(o):
        return top_third.at[pl.ds(pl.multiple_of(flip(x, o) * deep, deep), deep)]

    def finish():
        total = recv_third[0]
        for n in range(1, X):
            total = total + recv_third[n]
        fourth_in = relu_round(total)
        last_in = relu_round(dot_t(w4[...].reshape(last.shape[0], -1), fourth_in))
        out[...] = jnp.sum(last_in.astype(F32) * last[...], axis=0)

    def last_column():
        row = top_last[...].reshape(1, -1).astype(F32)
        last[...] = jnp.broadcast_to(row, (B, row.shape[1])).T

    for o in range(1, R):
        greet((me, flip(k, o)))
    get_idx = local(indices_h, indices, 0)
    get_len = local(lengths_h, bag_lengths, 1)

    @pl.when(core == 0)
    def follower():
        later = [local(top_fourth, w4.at[k], 2), local(top_last_h, top_last, 3)]
        get_idx.wait()
        get_len.wait()
        pair_idx[...] = own_tile()
        pl.semaphore_wait(barrier, R - 1)
        up = (me, mate)
        send(pair_idx, pair_idx, S_IDX, R_IDX, up)
        send(dense_h, dense.at[k], S_DENSE, R_DENSE, up)
        for o in range(1, X):
            lead = (me, flip(k, 2 * o + 1))
            send(dense_h, dense.at[k], S_DENSE, R_DENSE, lead)
            send(top_first, w1.at[k], S_W1, R_W1, lead)
            send(strip(o), w3.at[k], S_W3, R_W3, lead)
            send(top_fourth, w4.at[k], S_OWN, R_ACROSS + 2 * o, (me, flip(k, 2 * o)))
        send(top_first, w1.at[k], S_W1, R_W1, up)
        send(top_second, w2.at[0], S_W2, R_W2, up)
        send(strip(0), w3.at[k], S_W3, R_W3, up)
        send(top_fourth, w4.at[k], S_OWN, R_DOWN, up)
        if X > 1:
            arrive(w3.at[pl.ds(0, X - 1)], R_W3)
        for o in range(1, X):
            send(w3.at[o - 1], w3.at[mate], S_W3, R_W3, (me, flip(k, 2 * o + 1)))
        arrive(w4.at[mate], R_ACROSS)
        for o in range(1, X):
            send(w4.at[mate], w4.at[mate], S_FORWARD, R_ACROSS + 2 * o + 1, (me, flip(k, 2 * o)))
        for h in range(2):
            for o in range(1, X):
                block = w4.at[flip(k, 2 * o + h)]
                arrive(block, R_ACROSS + 2 * o + h)
                send(block, block, S_FORWARD, R_DOWN, up)
        for copy in later:
            copy.wait()
        last_column()
        arrive(recv_third, R_E4)
        finish()
        sent(pair_idx, S_IDX)
        sent(w2.at[0], S_W2)
        sent_blocks(dense, X, S_DENSE)
        sent_blocks(w1, X, S_W1)
        sent_blocks(w3, 2 * X - 1, S_W3)
        sent_blocks(w4, X, S_OWN)
        sent_blocks(w4, 3 * (X - 1), S_FORWARD)

    @pl.when(core == 1)
    def leader():
        for d in range(1, D):
            greet((flip(me, d), k))
        get_dense = local(dense_h, dense.at[k], 2)
        get_bottom = [
            local(bottom_first_h, bottom_first, 3),
            local(bottom_second_h, bottom_second, 4),
            local(bottom_third_h, bottom_third, 5),
        ]
        get_table = local(tables, table_v, 6)
        get_idx.wait()
        get_len.wait()
        later = [local(top_second, w2.at[1], 0), local(top_first, w1.at[k], 1)]
        mine = own_tile()
        pl.semaphore_wait(barrier, D - 1 + R - 1)
        arrive(pair_idx, R_IDX)
        out_idx[:, :HOT, :] = jnp.maximum(mine, pair_idx[...])

        for d in reversed(range(1, D)):
            peer = flip(me, d)
            send(
                out_idx.at[peer // per_table],
                recv_idx.at[me],
                S_E1,
                R_E1 + me // low,
                (peer, k),
            )
        recv_idx[me] = out_idx[me // per_table]
        for o in range(1, X):
            lead = (me, flip(k, 2 * o))
            send(dense_h, dense.at[k], S_DENSE, R_DENSE, lead)
            send(top_first, w1.at[k], S_W1, R_W1, lead)
            send(strip(o), w3.at[o - 1], S_W3, R_W3, (me, mate))
        send(top_fourth, w4.at[k], S_OWN, R_ACROSS, (me, mate))

        get_table.wait()
        table_t[...] = table_v[...].T

        offset = (me % per_table) * rows
        sub = lax.broadcasted_iota(jnp.int32, (PACK, LANES), 0)
        zero = jnp.zeros((PACK, LANES), BF16)

        def lookup(g):
            base = group * g
            entry = recv_idx[base, :HOT, :]
            for i in range(1, group):
                entry = jnp.maximum(entry, recv_idx[base + i, :HOT, :])
            codes, counts = [], []
            for s in range(HOT):
                row = jnp.broadcast_to(entry[s : s + 1, :], (PACK, LANES))
                spot = (row & (SPAN - 1)) - offset
                hit = jnp.logical_and((spot & (PACK - 1)) == sub, row >= 0)
                codes.append(jnp.where(hit, spot >> SHIFT, -1).astype(F32).astype(BF16))
                counts.append((row // SPAN).astype(F32).astype(BF16))
            partial = jnp.zeros((LANES, E), F32)
            for c in range(rows // CHUNK):
                chunk = []
                for n in range(c * CHUNK // PACK, (c + 1) * CHUNK // PACK):
                    total = zero
                    for code, count in zip(codes, counts):
                        total = jnp.where(code == jnp.asarray(n, BF16), count, total)
                    chunk.append(total)
                partial = partial + lax.dot_general(
                    jnp.concatenate(chunk, axis=0),
                    table_v[c * CHUNK : (c + 1) * CHUNK, :],
                    (((0,), (0,)), ((), ())),
                    preferred_element_type=F32,
                )
            part[pl.ds(base, group)] = partial.reshape(group, 2 * B, E)

        def run(base, count):
            if count == group:
                lookup(base // group)
            else:
                pl.loop(0, count // group)(lambda g: lookup(base // group + g))

        def back(peer, to, rsem):
            send(part.at[peer], recv_pool.at[x * D + me], S_E2, rsem, (peer, to))

        def second_send(r):
            if r < early:
                for o in range(1, X):
                    back(r, flip(k, 2 * o), R_E2X)
            else:
                second_send_straight(r)

        def second_send_straight(r):
            @pl.when(me != r)
            def straight():
                back(r, k, R_E2)

        for half in range(2):

            @pl.when(me // low == half)
            def from_own_half():
                arrive(recv_idx.at[pl.ds(0, low - 1)], R_E1 + half)

            @pl.when(me // low != half)
            def from_other_half():
                arrive(recv_idx.at[pl.ds(0, low)], R_E1 + half)

            run(half * low, low)
            for r in range(half * low, (half + 1) * low):
                second_send(r)
        recv_pool[x * D + me] = part[me]
        get_dense.wait()
        for copy in get_bottom:
            copy.wait()
        later += [
            local(strip(0), w3.at[k], 2),
            local(top_fourth, w4.at[k], 3),
            local(top_last_h, top_last, 4),
        ]
        arrive(dense.at[pl.ds(0, R - 1)], R_DENSE)
        arrive(w1.at[pl.ds(0, R - 1)], R_W1)
        lower = relu_round(dot(dense[...].reshape(R * B, -1), bottom_first[...]))
        middle = relu_round(dot(lower, bottom_second[...]))
        bottom_out = jnp.maximum(dot(middle, bottom_third[...]), 0.0)
        for r in range(early):
            second_send_straight(r)
        for copy in later:
            copy.wait()
        last_column()
        bottom[...] = bottom_out.reshape(X, 2 * B, E)
        bottom_in = bottom_out.astype(BF16)
        n1, n2 = w1.shape[2], w2.shape[2]
        for n in range(R):
            first[:, :, n * n1 : (n + 1) * n1] = dot(bottom_in, w1[n, :E, :]).reshape(
                X, 2 * B, n1
            )
        n3 = w3.shape[2]
        lane = lax.broadcasted_iota(jnp.int32, (2 * B, E), 1)

        def interact(y):
            features = [bottom[y]]
            for t in range(TAB):
                pooled = recv_pool[y * D + t * per_table]
                for i in range(1, per_table):
                    pooled = pooled + recv_pool[y * D + t * per_table + i]
                features.append(pooled)
            dots = jnp.zeros((2 * B, E), F32)
            p = 0
            for i in range(TAB + 1):
                for j in range(i + 1, TAB + 1):
                    value = jnp.sum(features[i] * features[j], axis=1, keepdims=True)
                    dots = jnp.where(lane == p, value, dots)
                    p += 1
            recv_dots[y] = dots.astype(BF16)

        def top(y):
            dots = recv_dots[y][:, : TAB * (TAB + 1) // 2]
            for n in range(R):
                act1[:, n * n1 : (n + 1) * n1] = relu_round(
                    first[y, :, n * n1 : (n + 1) * n1] + dot(dots, w1[n, E:, :])
                )
            act2 = jnp.concatenate([relu_round(dot(act1[...], w2[j])) for j in range(2)], axis=1)
            for n in range(R):
                third[pl.ds(2 * y, 2), :, n * n3 : (n + 1) * n3] = dot(act2, w3[n]).reshape(
                    2, B, n3
                )

        def weights():
            arrive(w2.at[0], R_W2)
            arrive(w3.at[pl.ds(0, R - 1)], R_W3)

        def others():
            for o in range(1, X):
                top(flip(x, o))
                for h in range(2):
                    to = flip(k, 2 * o + 1 - h)
                    send(third.at[to], recv_third.at[x], S_E4, R_E4, (me, to))

        def own():
            top(x)
            send(third.at[mate], recv_third.at[x], S_E4, R_E4, (me, mate))
            recv_third[x] = third[k]

        @pl.when(me < early)
        def ahead():
            if X > 1:
                arrive(recv_pool.at[pl.ds(0, (X - 1) * D)], R_E2X)
            for o in range(1, X):
                interact(flip(x, o))
            weights()
            others()
            arrive(recv_pool.at[pl.ds(0, D - 1)], R_E2)
            interact(x)
            own()

        @pl.when(me >= early)
        def behind():
            arrive(recv_pool.at[pl.ds(0, D - 1)], R_E2)
            interact(x)
            for o in range(1, X):
                send(recv_dots.at[x], recv_dots.at[x], S_E3, R_E3, (me, flip(k, 2 * o)))
            weights()
            own()
            if X > 1:
                arrive(recv_dots.at[pl.ds(0, X - 1)], R_E3)
            others()

        arrive(w4.at[pl.ds(0, R - 1)], R_DOWN)
        if X > 1:
            arrive(recv_third.at[pl.ds(0, X - 1)], R_E4)
        finish()
        sent(recv_idx.at[pl.ds(0, D - 1)], S_E1)
        sent_blocks(recv_pool, D - 1 + early * (X - 1), S_E2)
        sent(w4.at[k], S_OWN)
        sent(third.at[pl.ds(0, R - 1)], S_E4)
        if X > 1:
            sent_blocks(dense, X - 1, S_DENSE)
            sent_blocks(w1, X - 1, S_W1)
            sent_blocks(w3, X - 1, S_W3)

            @pl.when(me >= early)
            def sent_dots():
                sent(recv_dots.at[pl.ds(0, X - 1)], S_E3)


def body(*args):
    (tables, indices, bag_lengths, dense, b1, b2, b3, t1, t2, t3, t4, last) = args
    D = lax.axis_size("rows")
    R = lax.axis_size("rep")
    B = indices.shape[0]
    indices = jnp.transpose(indices, (1, 2, 0))
    bag_lengths = jnp.transpose(bag_lengths)
    t4 = jnp.transpose(t4)
    rows, E = tables.shape
    X = R // 2
    hbm = pl.BlockSpec(memory_space=pl.ANY)
    tile = pltpu.VMEM((TAB, HOT, LANES), jnp.int32)
    result = pl.pallas_call(
        functools.partial(kernel, D, R),
        out_shape=pltpu.VMEM((B,), F32),
        in_specs=[hbm] * 12,
        out_specs=pl.BlockSpec(memory_space=pltpu.VMEM),
        scratch_shapes=[
            pltpu.VMEM(indices.shape, jnp.int32),
            pltpu.VMEM(bag_lengths.shape, jnp.int32),
            pltpu.VMEM((R,) + dense.shape, BF16),
            pltpu.VMEM(b1.shape, BF16),
            pltpu.VMEM(b2.shape, BF16),
            pltpu.VMEM(b3.shape, BF16),
            pltpu.VMEM(last.shape, BF16),
            pltpu.VMEM((last.shape[0], B), F32),
            pltpu.VMEM((rows, E), BF16),
            pltpu.VMEM((E, rows), BF16),
            pltpu.VMEM((R,) + t1.shape, BF16),
            pltpu.VMEM((2,) + t2.shape, BF16),
            pltpu.VMEM((R, 2 * t2.shape[1], t3.shape[1]), BF16),
            pltpu.VMEM((R,) + t4.shape, BF16),
            tile,
            tile,
            pltpu.VMEM((TAB, HOT, LANES), jnp.int32),
            pltpu.VMEM((D, HOT, LANES), jnp.int32),
            pltpu.VMEM((D, 2 * B, E), F32),
            pltpu.VMEM((X * D, 2 * B, E), F32),
            pltpu.VMEM((X, 2 * B, E), BF16),
            pltpu.VMEM((X, 2 * B, E), F32),
            pltpu.VMEM((X, 2 * B, R * t1.shape[1]), F32),
            pltpu.VMEM((2 * B, R * t1.shape[1]), BF16),
            pltpu.VMEM((R, B, R * t3.shape[1]), F32),
            pltpu.VMEM((X, B, R * t3.shape[1]), F32),
            pltpu.SemaphoreType.DMA((max(27, R_ACROSS + R),)),
        ],
        compiler_params=pltpu.CompilerParams(collective_id=0, has_side_effects=True),
    )(tables, indices, bag_lengths, dense, b1, b2, b3, t1, t2, t3, t4, last)
    return result


def solution(mesh):
    placed = (
        P("rows", None),
        P(("rows", "rep"), None, None),
        P(("rows", "rep"), None),
        P(("rows", "rep"), None),
        P(),
        P(),
        P(),
        P(None, "rep"),
        P(None, "rep"),
        P(None, "rep"),
        P(None, "rep"),
        P(),
    )
    return jax.shard_map(
        body, mesh=mesh, in_specs=placed, out_specs=P(("rows", "rep")), check_vma=False
    )
```
